16 devices in a mesh: dp: 4 (over z, y), tp: 4 (over x, core).
Axes of the slice: x: 2, y: 2, z: 2, core: 2. Of those that a mesh axis runs over, the one named last changes fastest.
Arguments:
- x: bfloat16 [32768, 2048], P(('dp', 'tp')), parts along dimension 0
- dy: bfloat16 [32768, 2048], P(('dp', 'tp')), parts along dimension 0
- wg: bfloat16 [2048, 8192], P(None, 'tp')
- wu: bfloat16 [2048, 8192], P(None, 'tp')
- wd: bfloat16 [8192, 2048], P('tp')
Outputs:
- output 1: bfloat16 [32768, 2048], P(('dp', 'tp')), parts along dimension 0
- output 2: float32 [8192, 8192], P('dp', 'tp'), parts along dimension 0
- output 3: float32 [8192, 8192], P('dp', 'tp'), parts along dimension 0
- output 4: float32 [32768, 2048], P(('dp', 'tp')), parts along dimension 0
There are 4 independent parts. The reference program is written for one: setup_inputs(seed, part) draws one part's arguments, and reference() takes and returns one part's arrays. A program takes and returns all parts, laid end to end along the dimension named above; an argument that names none is the same for every part.
All inputs are finite; a program needn't handle non-finite values.
Results may differ from the reference program's by a relative error of at most 0.0102898.
Values are sent between devices in bfloat16 or wider.
A program may use at most 1 GiB of HBM per device.

```python
import jax
import jax.numpy as jnp

T = 8192
H = 2048
F = 8192


def setup_inputs(seed: int = 0, part: int = 0) -> dict:
    key = jax.random.PRNGKey(seed)
    kx, kdy = jax.random.split(jax.random.fold_in(key, part))
    kg, ku, kd = jax.random.split(key, 3)
    x = jax.random.normal(kx, (T, H), jnp.float32)
    dy = jax.random.normal(kdy, (T, H), jnp.float32)
    wg = jax.random.normal(kg, (H, F), jnp.float32) * H ** -0.5
    wu = jax.random.normal(ku, (H, F), jnp.float32) * H ** -0.5
    wd = jax.random.normal(kd, (F, H), jnp.float32) * F ** -0.5
    return {"x": x.astype(jnp.bfloat16), "dy": dy.astype(jnp.bfloat16),
            "wg": wg.astype(jnp.bfloat16), "wu": wu.astype(jnp.bfloat16),
            "wd": wd.astype(jnp.bfloat16)}


def _silu_and_grad(u):
    s = jax.nn.sigmoid(u)
    return u * s, s * (1.0 + u * (1.0 - s))


def reference(x, dy, wg, wu, wd):
    ug = jnp.dot(x, wg, preferred_element_type=jnp.float32).astype(jnp.bfloat16).astype(jnp.float32)
    uu = jnp.dot(x, wu, preferred_element_type=jnp.float32).astype(jnp.bfloat16).astype(jnp.float32)
    a, da = _silu_and_grad(ug)
    z = (a * uu).astype(jnp.bfloat16)
    dwd = jnp.dot(z.T, dy, preferred_element_type=jnp.float32)
    g = jnp.dot(dy, wd.T, preferred_element_type=jnp.float32)
    duu = (g * a).astype(jnp.bfloat16)
    dug = (g * uu * da).astype(jnp.bfloat16)
    p = jnp.dot(dug, wg.T, preferred_element_type=jnp.float32) + jnp.dot(duu, wu.T, preferred_element_type=jnp.float32)
    dx = p.astype(jnp.bfloat16)
    dwg = jnp.dot(x.T, dug, preferred_element_type=jnp.float32)
    dwu = jnp.dot(x.T, duu, preferred_element_type=jnp.float32)
    return dx, dwg, dwu, dwd
```

```python
import jax
import jax.numpy as jnp
from jax import lax
from jax.experimental import pallas as pl
from jax.experimental.pallas import tpu as pltpu
from jax.sharding import PartitionSpec as P

F32, BF16 = jnp.float32, jnp.bfloat16
NN = (((1,), (0,)), ((), ()))
NT = (((1,), (1,)), ((), ()))
TN = (((0,), (0,)), ((), ()))
ANY = pl.BlockSpec(memory_space=pl.ANY)
MESH = pl.DeviceIdType.MESH
DMA = pltpu.SemaphoreType.DMA

S = 2048
T = 1024
C = 512
SUB = 256
VMEM = 67043328


def _dot(a, b, dims):
    return lax.dot_general(a, b, dims, preferred_element_type=F32)


def _ds(i, n):
    return pl.ds(pl.multiple_of(i * n, n), n)


def _gate(la, lb, wn, wt, ob):
    for i in range(T // SUB):
        r = pl.ds(i * SUB, SUB)
        ug = _dot(la[r, :], wn[:, pl.ds(0, C)], NN).astype(BF16).astype(F32)
        uu = _dot(la[r, :], wn[:, pl.ds(C, C)], NN).astype(BF16).astype(F32)
        g = _dot(lb[r, :], wt[...], NT)
        s = jax.nn.sigmoid(ug)
        a = ug * s
        ob[0, r, :] = (a * uu).astype(BF16)
        ob[1, r, :] = (g * uu * (s * (1.0 + ug * (1.0 - s)))).astype(BF16)
        ob[2, r, :] = (g * a).astype(BF16)


def _wdot(la, wn):
    return _dot(la[:, pl.ds(0, T)], wn[pl.ds(0, T), :], TN) + _dot(la[:, pl.ds(T, T)], wn[pl.ds(T, T), :], TN)


def _k1(x, dy, wg, wu, wd, xa, dya, z, dug, duu, psib, s01, s23, r01, pg, pu, pd,
        la, lb, wn, wt, ob, acc, rcv, lsem, rsem, osem, asem,
        far_s, far_r, sib_s, sib_r, fwd_s, fwd_r, p_s, p_r, s_s, s_r):
    me = lax.axis_index("tp")
    sib = me // 2 * 2 + 1 - me % 2
    far = (me + 2) % 4
    copy = pltpu.make_async_copy

    def remote(src, dst, ss, rs, dev):
        return pltpu.make_async_remote_copy(src_ref=src, dst_ref=dst, send_sem=ss, recv_sem=rs,
                                            device_id={"tp": dev}, device_id_type=MESH)

    def far_copy(q, j):
        src, dst = ((x, xa), (dy, dya))[j]
        return remote(src.at[pl.ds(q * C, C)], dst.at[pl.ds(S + q * T, C)], far_s.at[2 * q + j], far_r.at[2 * q + j], far)

    def sib_copy(j):
        src, dst = ((x, xa), (dy, dya))[j]
        return remote(src, dst.at[pl.ds(0, S)], sib_s.at[j], sib_r.at[j], sib)

    def fwd_copy(q, j):
        buf = (xa, dya)[j]
        return remote(buf.at[pl.ds(S + q * T, C)], buf.at[pl.ds(S + q * T + C, C)], fwd_s.at[2 * q + j], fwd_r.at[2 * q + j], sib)

    def forward(q):
        for j in range(2):
            far_copy(q, j).wait_recv()
            fwd_copy(q, j).start()

    def s_copy():
        return remote(s01, r01, s_s.at[0], s_r.at[0], far)

    def f_lhs(t, slot):
        def go(a, b, row):
            copy(a.at[_ds(row, T)], la.at[slot], lsem.at[slot, 0]).start()
            copy(b.at[_ds(row, T)], lb.at[slot], lsem.at[slot, 1]).start()
        pl.when(t < 2)(lambda: go(x, dy, t))
        pl.when(t >= 2)(lambda: go(xa, dya, t - 2))

    def f_lhs_wait(slot):
        copy(x.at[pl.ds(0, T)], la.at[slot], lsem.at[slot, 0]).wait()
        copy(dy.at[pl.ds(0, T)], lb.at[slot], lsem.at[slot, 1]).wait()

    def f_rhs(n, slot):
        return (copy(wg.at[:, _ds(n, C)], wn.at[slot, :, pl.ds(0, C)], rsem.at[slot, 0]),
                copy(wu.at[:, _ds(n, C)], wn.at[slot, :, pl.ds(C, C)], rsem.at[slot, 1]),
                copy(wd.at[_ds(n, C)], wt.at[slot, 0], rsem.at[slot, 2]))

    def f_outs(t, n, slot):
        return [copy(ob.at[slot, j], dst.at[_ds(t, T), _ds(n, C)], osem.at[slot, j]) for j, dst in enumerate((z, dug, duu))]

    def d_lhs(blk, g, slot):
        for j in range(2):
            row = jnp.where(blk == 1, 4 + 2 * g + j, 8 + 2 * (2 * (blk - 2) + j) + 1 - g)
            copy(dug.at[_ds(row, C)], la.at[slot, pl.ds(j * C, C)], lsem.at[slot, 2 * j]).start()
            copy(duu.at[_ds(row, C)], lb.at[slot, pl.ds(j * C, C)], lsem.at[slot, 2 * j + 1]).start()

    def d_lhs_wait(slot):
        for j in range(2):
            copy(dug.at[pl.ds(0, C)], la.at[slot, pl.ds(j * C, C)], lsem.at[slot, 2 * j]).wait()
            copy(duu.at[pl.ds(0, C)], lb.at[slot, pl.ds(j * C, C)], lsem.at[slot, 2 * j + 1]).wait()

    def d_rhs(n, slot):
        return (copy(wg.at[_ds(n, C)], wt.at[slot, 0], rsem.at[slot, 0]),
                copy(wu.at[_ds(n, C)], wt.at[slot, 1], rsem.at[slot, 1]))

    def d_rcv(blk, n, slot):
        return copy(psib.at[_ds(blk, T), _ds(n, C)], rcv.at[slot], rsem.at[slot, 2])

    def d_send(blk, g, n, slot):
        row = jnp.where(blk == 1, g, blk)
        tile = jnp.where(blk == 1, 4 * g, 4 * blk) + n
        return remote(ob.at[slot, 0], psib.at[_ds(row, T), _ds(n, C)], p_s.at[slot], p_r.at[tile], sib)

    def d_out(dst, n, slot):
        return copy(ob.at[slot, 0], dst.at[:, _ds(n, C)], osem.at[slot, 0])

    def d_prefetch(blk, i):
        slot = i % 2
        for c in d_rhs(i % 4, slot):
            c.start()

        @pl.when((blk > 1) & (i >= 4))
        def _():
            d_send(blk, 0, i - 4, slot).wait_recv()
            d_rcv(blk, i - 4, slot).start()

    def w_of(blk, grp):
        h = jnp.where(blk == 3, 5, grp)
        unit = jnp.where(blk == 1, grp // 2, 4 + h // 3)
        k = jnp.where(blk == 1, grp % 2, h % 3)
        return unit, k

    def w_lhs(unit, k, slot):
        m = unit % 2

        def go(src, row):
            for j in range(2):
                copy(src.at[_ds(2 * row + j, T), _ds(m, T)], la.at[slot, :, pl.ds(j * T, T)], lsem.at[slot, j]).start()
        pl.when((unit < 4) & (k == 0))(lambda: go(x, 0))
        pl.when((unit < 4) & (k > 0))(lambda: go(xa, k - 1))
        pl.when(unit >= 4)(lambda: go(z, k))

    def w_lhs_wait(slot):
        for j in range(2):
            copy(x.at[pl.ds(0, T), pl.ds(0, T)], la.at[slot, :, pl.ds(j * T, T)], lsem.at[slot, j]).wait()

    def w_rhs(unit, k, n):
        def go(src, row):
            copy(src.at[_ds(row, S), _ds(n, T)], wn.at[n], rsem.at[n, 0]).start()
        pl.when(unit < 2)(lambda: go(dug, k))
        pl.when((unit >= 2) & (unit < 4))(lambda: go(duu, k))
        pl.when((unit >= 4) & (k == 0))(lambda: go(dy, 0))
        pl.when((unit >= 4) & (k > 0))(lambda: go(dya, k - 1))

    def w_rhs_wait(n):
        copy(x.at[:, pl.ds(0, T)], wn.at[n], rsem.at[n, 0]).wait()

    def w_out(unit, n):
        def go(dst):
            copy(acc.at[n], dst.at[_ds(unit % 2, T), _ds(n, T)], asem.at[n]).start()
        pl.when(unit < 2)(lambda: go(pg))
        pl.when((unit >= 2) & (unit < 4))(lambda: go(pu))
        pl.when(unit >= 4)(lambda: go(pd))

    def w_out_wait(n):
        copy(acc.at[n], pg.at[pl.ds(0, T), pl.ds(0, T)], asem.at[n]).wait()

    f_lhs(0, 0)
    for c in f_rhs(0, 0):
        c.start()
    rcv[...] = jnp.zeros_like(rcv)
    bar = pltpu.get_barrier_semaphore()
    for dev in (sib, far):
        pl.semaphore_signal(bar, inc=1, device_id={"tp": dev}, device_id_type=MESH)
    pl.semaphore_wait(bar, 2)
    for q in range(4):
        for j in range(2):
            far_copy(q, j).start()
    for j in range(2):
        sib_copy(j).start()

    def block(blk, carry):
        odd = jnp.where(blk == 3, 1, 0)
        dodd = jnp.where(blk == 2, 1, 0)
        n_w = jnp.where(blk == 1, 8, jnp.where(blk == 2, 5, jnp.where(blk == 3, 1, 0)))

        def f_step(i, carry):
            t, n, slot = 2 * blk + i // 4, i % 4, i % 2
            ls = (i // 4 + odd) % 2

            @pl.when((blk == 3) & (i == 3))
            def _():
                forward(3)

            @pl.when((blk == 3) & (i == 4))
            def _():
                for j in range(2):
                    fwd_copy(3, j).wait_recv()
                f_lhs(t, ls)
            pl.when(n == 0)(lambda: f_lhs_wait(ls))
            for c in f_rhs(n, slot):
                c.wait()

            @pl.when((i < 7) | (blk == 0))
            def _():
                for c in f_rhs((n + 1) % 4, 1 - slot):
                    c.start()

            @pl.when((n == 3) & ((i == 7) & (blk == 0) | (i == 3) & (blk < 3)))
            def _():
                @pl.when((blk == 0) & (i == 7))
                def _():
                    for j in range(2):
                        sib_copy(j).wait_recv()

                @pl.when(blk == 2)
                def _():
                    for j in range(2):
                        fwd_copy(1, j).wait_recv()
                f_lhs(t + 1, 1 - ls)

            @pl.when((i == 7) & (blk > 0))
            def _():
                unit, k = w_of(blk, 0)
                w_lhs(unit, k, 1 - ls)
                w_rhs(unit, k, 0)

            @pl.when((i >= 2) | (blk == 1))
            def _():
                for c in f_outs(t, n, slot):
                    c.wait()

            @pl.when((i < 2) & (blk == 2))
            def _():
                d_send(1, 1, 2 + i, slot).wait_send()

            @pl.when((i < 2) & (blk == 3))
            def _():
                d_out(s01, 2 + i, slot).wait()
                pl.when(i == 1)(lambda: s_copy().start())

            _gate(la.at[ls], lb.at[ls], wn.at[slot], wt.at[slot, 0], ob.at[slot])
            for c in f_outs(t, n, slot):
                c.start()
            return carry

        lax.fori_loop(0, 8, f_step, 0)

        def w_step(i, carry):
            grp, n = i // 2, i % 2
            unit, k = w_of(blk, grp)
            ls = (grp + odd) % 2
            last = jnp.where(unit < 4, 1, 2)

            @pl.when((blk == 1) & (i == 0))
            def _():
                forward(0)

            @pl.when((blk == 2) & (i == 3))
            def _():
                forward(2)
            pl.when(n == 0)(lambda: w_lhs_wait(ls))
            w_rhs_wait(n)

            @pl.when(i == 1)
            def _():
                for s in range(2):
                    for c in f_outs(0, 0, s):
                        c.wait()

            @pl.when(n == 0)
            def _():
                w_rhs(unit, k, 1)

                @pl.when(grp + 1 < n_w)
                def _():
                    unit2, k2 = w_of(blk, grp + 1)
                    w_lhs(unit2, k2, 1 - ls)

            @pl.when(n == 1)
            def _():
                @pl.when(grp + 1 < n_w)
                def _():
                    unit2, k2 = w_of(blk, grp + 1)
                    w_rhs(unit2, k2, 0)

                @pl.when(grp + 1 == n_w)
                def _():
                    d_lhs(blk, 0, 1 - ls)
                    d_prefetch(blk, 0)
            pl.when((k == 0) & (unit > 0))(lambda: w_out_wait(n))
            acc[n] = jnp.where(k == 0, 0.0, acc[n]) + _wdot(la.at[ls], wn.at[n])
            pl.when(k == last)(lambda: w_out(unit, n))
            return carry

        lax.fori_loop(0, 2 * n_w, w_step, 0)

        def d_step(i, carry):
            g, n, slot = i // 4, i % 4, i % 2
            ls = (g + dodd) % 2
            mine = (blk > 1) & (g == 1)

            @pl.when((blk == 1) & (i == 3))
            def _():
                forward(1)
            pl.when(n == 0)(lambda: d_lhs_wait(ls))
            for c in d_rhs(n, slot):
                c.wait()
            pl.when(mine)(lambda: d_rcv(blk, n, slot).wait())

            pl.when(i == 2)(lambda: d_lhs(blk, 1, 1 - ls))
            pl.when(i < 7)(lambda: d_prefetch(blk, i + 1))

            @pl.when((i == 6) & (blk < 3))
            def _():
                @pl.when(blk == 1)
                def _():
                    for j in range(2):
                        fwd_copy(0, j).wait_recv()

                @pl.when(blk == 2)
                def _():
                    for j in range(2):
                        fwd_copy(2, j).wait_recv()
                f_lhs(2 * blk + 2, 1 - ls)

            @pl.when((i == 7) & (blk < 3))
            def _():
                for c in f_rhs(0, 0):
                    c.start()

            pl.when((i >= 2) & ((blk == 1) | (i < 6)))(lambda: d_send(blk, 0, 0, slot).wait_send())
            pl.when((i >= 6) & (blk > 1))(lambda: d_out(s01, n, slot).wait())

            p = _dot(la[ls], wt[slot, 0], NT) + _dot(lb[ls], wt[slot, 1], NT)
            ob[slot, 0] = (p + jnp.where(mine, rcv[slot].astype(F32), 0.0)).astype(BF16)
            pl.when(~mine)(lambda: d_send(blk, g, n, slot).start())
            pl.when(mine & (blk == 2))(lambda: d_out(s01, n, slot).start())
            pl.when(mine & (blk == 3))(lambda: d_out(s23, n, slot).start())
            return carry

        @pl.when(blk > 0)
        def _():
            lax.fori_loop(0, 8, d_step, 0)
        return carry

    lax.fori_loop(0, 4, block, 0)

    for s in range(2):
        d_out(s23, 2 + s, s).wait()
        w_out_wait(s)
    for j in range(2):
        sib_copy(j).wait_send()
        for q in range(4):
            far_copy(q, j).wait_send()
            fwd_copy(q, j).wait_send()
    for i in range(8):
        d_send(1, i // 4, i % 4, i % 2).wait_recv()
    s_copy().wait()


def _k2(x_, dya, xa, z, dug, duu, psib, r01, wg, wu, pg, pu, pd, dwg, dwu, dwd, dx,
        la, lb, wn, wt, ob, acc, add, lsem, rsem, osem, asem, psem, dsem):
    del x_
    copy = pltpu.make_async_copy
    n_w = 10

    def w_of(grp):
        unit = jnp.where(grp < 8, grp // 2, grp - 4)
        k = jnp.where(grp < 8, 2 + grp % 2, 3)
        return unit, k

    def w_lhs(unit, k, slot):
        def go(src, row):
            for j in range(2):
                copy(src.at[_ds(2 * row + j, T), _ds(unit % 2, T)], la.at[slot, :, pl.ds(j * T, T)], lsem.at[slot, j]).start()
        pl.when(unit < 4)(lambda: go(xa, k - 1))
        pl.when(unit >= 4)(lambda: go(z, k))

    def w_lhs_wait(slot):
        for j in range(2):
            copy(xa.at[pl.ds(0, T), pl.ds(0, T)], la.at[slot, :, pl.ds(j * T, T)], lsem.at[slot, j]).wait()

    def w_rhs(unit, k, n):
        def go(src, row):
            copy(src.at[_ds(row, S), _ds(n, T)], wn.at[n], rsem.at[n, 0]).start()
        pl.when(unit < 2)(lambda: go(dug, k))
        pl.when((unit >= 2) & (unit < 4))(lambda: go(duu, k))
        pl.when(unit >= 4)(lambda: go(dya, k - 1))

    def w_rhs_wait(n):
        copy(dug.at[pl.ds(0, S), pl.ds(0, T)], wn.at[n], rsem.at[n, 0]).wait()

    def w_part(unit, n):
        a = 2 * (unit % 2) + n

        def go(src):
            copy(src.at[_ds(unit % 2, T), _ds(n, T)], acc.at[a], psem.at[a]).start()
        pl.when(unit < 2)(lambda: go(pg))
        pl.when((unit >= 2) & (unit < 4))(lambda: go(pu))
        pl.when(unit >= 4)(lambda: go(pd))

    def w_part_wait(a):
        copy(pg.at[pl.ds(0, T), pl.ds(0, T)], acc.at[a], psem.at[a]).wait()

    def w_out(unit, n):
        a = 2 * (unit % 2) + n

        def go(dst):
            copy(acc.at[a], dst.at[_ds(unit % 2, T), _ds(n, T)], asem.at[a]).start()
        pl.when(unit < 2)(lambda: go(dwg))
        pl.when((unit >= 2) & (unit < 4))(lambda: go(dwu))
        pl.when(unit >= 4)(lambda: go(dwd))

    def w_out_wait(a):
        copy(acc.at[a], dwg.at[pl.ds(0, T), pl.ds(0, T)], asem.at[a]).wait()

    def d_lhs(slot):
        return (copy(dug.at[pl.ds(0, T)], la.at[slot], lsem.at[slot, 0]),
                copy(duu.at[pl.ds(0, T)], lb.at[slot], lsem.at[slot, 1]))

    def d_rhs(n, slot):
        return (copy(wg.at[_ds(n, C)], wt.at[slot, 0], rsem.at[slot, 0]),
                copy(wu.at[_ds(n, C)], wt.at[slot, 1], rsem.at[slot, 1]),
                copy(psib.at[pl.ds(0, T), _ds(n, C)], add.at[slot, 0], dsem.at[slot, 0]),
                copy(r01.at[:, _ds(n, C)], add.at[slot, 1], dsem.at[slot, 1]))

    def d_out(n, slot):
        return copy(ob.at[slot], dx.at[pl.ds(0, T), _ds(n, C)], osem.at[slot])

    w_lhs(0, 2, 0)
    w_rhs(0, 2, 0)
    for n in range(2):
        w_part(0, n)

    def w_step(i, carry):
        grp, n = i // 2, i % 2
        unit, k = w_of(grp)
        ls = grp % 2
        a = 2 * (unit % 2) + n
        first = (grp >= 8) | (k == 2)
        pl.when(n == 0)(lambda: w_lhs_wait(ls))
        w_rhs_wait(n)

        @pl.when(n == 0)
        def _():
            w_rhs(unit, k, 1)

            @pl.when(grp + 1 < n_w)
            def _():
                unit2, k2 = w_of(grp + 1)
                w_lhs(unit2, k2, 1 - ls)

            @pl.when(grp + 1 == n_w)
            def _():
                for c in d_lhs(1 - ls):
                    c.start()

        @pl.when(n == 1)
        def _():
            @pl.when(grp + 1 < n_w)
            def _():
                unit2, k2 = w_of(grp + 1)
                w_rhs(unit2, k2, 0)

            @pl.when(grp + 1 == n_w)
            def _():
                for c in d_rhs(0, 0):
                    c.start()

        @pl.when(first)
        def _():
            w_part_wait(a)

            @pl.when(unit < 5)
            def _():
                b = 2 * ((unit + 1) % 2) + n
                pl.when(unit > 0)(lambda: w_out_wait(b))
                w_part(unit + 1, n)
        acc[a] = acc[a] + _wdot(la.at[ls], wn.at[n])
        pl.when(k == 3)(lambda: w_out(unit, n))
        return carry

    lax.fori_loop(0, 2 * n_w, w_step, 0)

    def d_step(n, carry):
        slot = n % 2
        pl.when(n == 0)(lambda: [c.wait() for c in d_lhs(0)] and None)
        for c in d_rhs(n, slot):
            c.wait()

        @pl.when(n < 3)
        def _():
            for c in d_rhs(n + 1, 1 - slot):
                c.start()
        pl.when(n >= 2)(lambda: d_out(n, slot).wait())
        p = _dot(la[0], wt[slot, 0], NT) + _dot(lb[0], wt[slot, 1], NT)
        ob[slot] = (p + add[slot, 0].astype(F32) + add[slot, 1].astype(F32)).astype(BF16)
        d_out(n, slot).start()
        return carry

    lax.fori_loop(0, 4, d_step, 0)
    for s in range(2):
        d_out(2 + s, s).wait()
    for a in range(4):
        w_out_wait(a)


def _k3(dug, duu, wg, wu, p1, p2, _, dx):
    p = _dot(dug[...], wg[...], NT) + _dot(duu[...], wu[...], NT)
    dx[...] = (p + p1[...].astype(F32) + p2[...].astype(F32)).astype(BF16)


def _local(x, dy, wg, wu, wd):
    def bf(r):
        return jax.ShapeDtypeStruct((r, S), BF16)

    def ff(r):
        return jax.ShapeDtypeStruct((r, S), F32)
    k1 = pl.pallas_call(
        _k1, name="gather_gate",
        out_shape=(bf(3 * S), bf(3 * S), bf(4 * S), bf(4 * S), bf(4 * S), bf(2 * S), bf(T), bf(T), bf(T), ff(S), ff(S), ff(S)),
        in_specs=[ANY] * 5, out_specs=(ANY,) * 12,
        scratch_shapes=[pltpu.VMEM((2, T, S), BF16), pltpu.VMEM((2, T, S), BF16), pltpu.VMEM((2, S, T), BF16),
                        pltpu.VMEM((2, 2, C, S), BF16), pltpu.VMEM((2, 3, T, C), BF16), pltpu.VMEM((2, T, T), F32),
                        pltpu.VMEM((2, T, C), BF16), DMA((2, 4)), DMA((2, 3)), DMA((2, 3)), DMA((2,)),
                        DMA((8,)), DMA((8,)), DMA((2,)), DMA((2,)), DMA((8,)), DMA((8,)), DMA((2,)), DMA((16,)),
                        DMA((1,)), DMA((1,))],
        cost_estimate=pl.CostEstimate(flops=420_000_000_000, bytes_accessed=1 << 30, transcendentals=0),
        compiler_params=pltpu.CompilerParams(collective_id=0, has_side_effects=True, vmem_limit_bytes=VMEM))
    xa, dya, z, dug, duu, psib, _, s23, r01, pg, pu, pd = k1(x, dy, wg, wu, wd)
    r23 = lax.ppermute(s23, "tp", [(0, 2), (2, 0), (1, 3), (3, 1)])
    k2 = pl.pallas_call(
        _k2, name="wgrad_dx",
        out_shape=(ff(S), ff(S), ff(S), bf(S)),
        in_specs=[ANY] * 13, out_specs=(ANY,) * 4,
        scratch_shapes=[pltpu.VMEM((2, T, S), BF16), pltpu.VMEM((1, T, S), BF16), pltpu.VMEM((2, S, T), BF16),
                        pltpu.VMEM((2, 2, C, S), BF16), pltpu.VMEM((2, T, C), BF16), pltpu.VMEM((4, T, T), F32),
                        pltpu.VMEM((2, 2, T, C), BF16), DMA((2, 2)), DMA((2, 2)), DMA((2,)), DMA((4,)), DMA((4,)), DMA((2, 2))],
        cost_estimate=pl.CostEstimate(flops=105_000_000_000, bytes_accessed=1 << 28, transcendentals=0),
        compiler_params=pltpu.CompilerParams(vmem_limit_bytes=VMEM))
    dwg, dwu, dwd, dx = k2(x, dya, xa, z, dug, duu, psib, r01, wg, wu, pg, pu, pd)
    row = pl.BlockSpec((T, S), lambda n: (1, 0))
    col = pl.BlockSpec((C, S), lambda n: (n, 0))
    tile = pl.BlockSpec((T, C), lambda n: (1, n))
    dx = pl.pallas_call(
        _k3, name="dx", out_shape=bf(S), grid=(S // C,),
        in_specs=[row, row, col, col, tile, pl.BlockSpec((T, C), lambda n: (0, n)), ANY],
        out_specs=tile, input_output_aliases={6: 0},
        cost_estimate=pl.CostEstimate(flops=4 * T * S * S, bytes_accessed=1 << 25, transcendentals=0),
        compiler_params=pltpu.CompilerParams(vmem_limit_bytes=60 << 20))(dug, duu, wg, wu, psib, r23, dx)
    return dx, dwg, dwu, dwd


def solution(mesh):
    rows = P(("dp", "tp"), None)
    return jax.shard_map(_local, mesh=mesh,
                         in_specs=(rows, rows, P(None, "tp"), P(None, "tp"), P("tp", None)),
                         out_specs=(rows, P("dp", "tp"), P("dp", "tp"), rows),
                         check_vma=False)
```

```python
import jax
import jax.numpy as jnp
from jax import lax
from jax.experimental import pallas as pl
from jax.experimental.pallas import tpu as pltpu
from jax.sharding import PartitionSpec as P

F32, BF16 = jnp.float32, jnp.bfloat16
NN = (((1,), (0,)), ((), ()))
NT = (((1,), (1,)), ((), ()))
TN = (((0,), (0,)), ((), ()))
ANY = pl.BlockSpec(memory_space=pl.ANY)
MESH = pl.DeviceIdType.MESH
DMA = pltpu.SemaphoreType.DMA

S = 2048
T = 1024
C = 512
VMEM = 67043328


def _dot(a, b, dims):
    return lax.dot_general(a, b, dims, preferred_element_type=F32)


def _ds(i, n):
    return pl.ds(pl.multiple_of(i * n, n), n)


def _gate(la, lb, wn, wt, ob):
    g = _dot(lb[...], wt[...], NT)
    ug = _dot(la[...], wn[:, pl.ds(0, C)], NN).astype(BF16).astype(F32)
    s = jax.nn.sigmoid(ug)
    a = ug * s
    ob[2] = (g * a).astype(BF16)
    gd = g * (s * (1.0 + ug * (1.0 - s)))
    uu = _dot(la[...], wn[:, pl.ds(C, C)], NN).astype(BF16).astype(F32)
    ob[0] = (a * uu).astype(BF16)
    ob[1] = (gd * uu).astype(BF16)


def _wgrad(acc, base, la, wn, lb, keep):
    a0, a1 = la[:, pl.ds(0, T)], la[:, pl.ds(T, T)]
    rhs = ((wn[pl.ds(0, T), :], wn[pl.ds(T, T), :]), (lb[:, pl.ds(0, T)], lb[:, pl.ds(T, T)]))
    for n in range(2):
        old = acc[base + n]
        old = old if keep is None else jnp.where(keep, old, 0.0)
        acc[base + n] = old + _dot(a0, rhs[n][0], TN) + _dot(a1, rhs[n][1], TN)


def _k1(x, dy, wg, wu, wd, xa, dya, z, dug, duu, psib, s01, s23, r01, pg, pu, pd,
        la, lb, wn, wt, ob, acc, rcv, lsem, rsem, osem, asem,
        far_s, far_r, sib_s, sib_r, fwd_s, fwd_r, p_s, p_r, s_s, s_r):
    me = lax.axis_index("tp")
    sib = me // 2 * 2 + 1 - me % 2
    far = (me + 2) % 4
    copy = pltpu.make_async_copy

    def remote(src, dst, ss, rs, dev):
        return pltpu.make_async_remote_copy(src_ref=src, dst_ref=dst, send_sem=ss, recv_sem=rs,
                                            device_id={"tp": dev}, device_id_type=MESH)

    def far_copy(q, j):
        src, dst = ((x, xa), (dy, dya))[j]
        return remote(src.at[pl.ds(q * C, C)], dst.at[pl.ds(S + q * T, C)], far_s.at[2 * q + j], far_r.at[2 * q + j], far)

    def sib_copy(j):
        src, dst = ((x, xa), (dy, dya))[j]
        return remote(src, dst.at[pl.ds(0, S)], sib_s.at[j], sib_r.at[j], sib)

    def fwd_copy(q, j):
        buf = (xa, dya)[j]
        return remote(buf.at[pl.ds(S + q * T, C)], buf.at[pl.ds(S + q * T + C, C)], fwd_s.at[2 * q + j], fwd_r.at[2 * q + j], sib)

    def forward(q):
        for j in range(2):
            far_copy(q, j).wait_recv()
            fwd_copy(q, j).start()

    def s_copy():
        return remote(s01, r01, s_s.at[0], s_r.at[0], far)

    def f_lhs(t, slot):
        def go(a, b, row):
            copy(a.at[_ds(row, T)], la.at[slot], lsem.at[slot, 0]).start()
            copy(b.at[_ds(row, T)], lb.at[slot], lsem.at[slot, 1]).start()
        pl.when(t < 2)(lambda: go(x, dy, t))
        pl.when(t >= 2)(lambda: go(xa, dya, t - 2))

    def f_lhs_wait(slot):
        copy(x.at[pl.ds(0, T)], la.at[slot], lsem.at[slot, 0]).wait()
        copy(dy.at[pl.ds(0, T)], lb.at[slot], lsem.at[slot, 1]).wait()

    def f_rhs(n, slot):
        return (copy(wg.at[:, _ds(n, C)], wn.at[slot, :, pl.ds(0, C)], rsem.at[slot, 0]),
                copy(wu.at[:, _ds(n, C)], wn.at[slot, :, pl.ds(C, C)], rsem.at[slot, 1]),
                copy(wd.at[_ds(n, C)], wt.at[slot, 0], rsem.at[slot, 2]))

    def f_outs(t, n, slot):
        return [copy(ob.at[slot, j], dst.at[_ds(t, T), _ds(n, C)], osem.at[slot, j]) for j, dst in enumerate((z, dug, duu))]

    def d_lhs(blk, g, slot):
        for j in range(2):
            row = jnp.where(blk == 1, 4 + 2 * g + j, 8 + 2 * (2 * (blk - 2) + j) + 1 - g)
            copy(dug.at[_ds(row, C)], la.at[slot, pl.ds(j * C, C)], lsem.at[slot, 2 * j]).start()
            copy(duu.at[_ds(row, C)], lb.at[slot, pl.ds(j * C, C)], lsem.at[slot, 2 * j + 1]).start()

    def d_lhs_wait(slot):
        for j in range(2):
            copy(dug.at[pl.ds(0, C)], la.at[slot, pl.ds(j * C, C)], lsem.at[slot, 2 * j]).wait()
            copy(duu.at[pl.ds(0, C)], lb.at[slot, pl.ds(j * C, C)], lsem.at[slot, 2 * j + 1]).wait()

    def d_rhs(n, slot):
        return [copy(wg.at[_ds(n, T), pl.ds(j * T, T)], wn.at[slot, pl.ds(j * T, T)], rsem.at[slot, j]) for j in range(2)] + [
            copy(wu.at[_ds(2 * n + j, C)], wt.at[slot, j], rsem.at[slot, 2 + j]) for j in range(2)]

    def d_send_own(g, n, slot, h):
        return remote(ob.at[slot, h], psib.at[_ds(g, T), _ds(2 * n + h, C)], p_s.at[slot, h], p_r.at[4 * g + 2 * n + h], sib)

    def d_send_far(blk, n, slot, h):
        return remote(ob.at[slot, h], rcv.at[2 * n + h], p_s.at[slot, h], p_r.at[4 * blk + 2 * n + h], sib)

    def d_out(dst, n, slot, h):
        return copy(ob.at[slot, h], dst.at[:, _ds(2 * n + h, C)], osem.at[slot, h])

    def w_of(blk, grp):
        h = jnp.where(blk == 3, 5, grp)
        unit = jnp.where(blk == 1, grp // 2, 4 + h // 3)
        k = jnp.where(blk == 1, grp % 2, h % 3)
        return unit, k

    def w_lhs(unit, k, slot):
        m = unit % 2

        def go(src, row):
            for j in range(2):
                copy(src.at[_ds(2 * row + j, T), _ds(m, T)], la.at[slot, :, pl.ds(j * T, T)], lsem.at[slot, j]).start()
        pl.when((unit < 4) & (k == 0))(lambda: go(x, 0))
        pl.when((unit < 4) & (k > 0))(lambda: go(xa, k - 1))
        pl.when(unit >= 4)(lambda: go(z, k))

    def w_lhs_wait(slot):
        for j in range(2):
            copy(x.at[pl.ds(0, T), pl.ds(0, T)], la.at[slot, :, pl.ds(j * T, T)], lsem.at[slot, j]).wait()

    def w_rhs(unit, k, slot):
        def go(src, row):
            copy(src.at[_ds(row, S), pl.ds(0, T)], wn.at[slot], rsem.at[slot, 0]).start()
            for j in range(2):
                copy(src.at[_ds(2 * row + j, T), pl.ds(T, T)], lb.at[slot, :, pl.ds(j * T, T)], rsem.at[slot, 1 + j]).start()
        pl.when(unit < 2)(lambda: go(dug, k))
        pl.when((unit >= 2) & (unit < 4))(lambda: go(duu, k))
        pl.when((unit >= 4) & (k == 0))(lambda: go(dy, 0))
        pl.when((unit >= 4) & (k > 0))(lambda: go(dya, k - 1))

    def w_rhs_wait(slot):
        copy(x.at[:, pl.ds(0, T)], wn.at[slot], rsem.at[slot, 0]).wait()
        for j in range(2):
            copy(x.at[pl.ds(0, T), pl.ds(0, T)], lb.at[slot, :, pl.ds(j * T, T)], rsem.at[slot, 1 + j]).wait()

    def w_out(unit):
        def go(dst):
            for n in range(2):
                copy(acc.at[n], dst.at[_ds(unit % 2, T), pl.ds(n * T, T)], asem.at[n]).start()
        pl.when(unit < 2)(lambda: go(pg))
        pl.when((unit >= 2) & (unit < 4))(lambda: go(pu))
        pl.when(unit >= 4)(lambda: go(pd))

    def w_out_wait(n):
        copy(acc.at[n], pg.at[pl.ds(0, T), pl.ds(0, T)], asem.at[n]).wait()

    f_lhs(0, 0)
    for c in f_rhs(0, 0):
        c.start()
    rcv[4] = jnp.zeros_like(rcv[4])
    bar = pltpu.get_barrier_semaphore()
    for dev in (sib, far):
        pl.semaphore_signal(bar, inc=1, device_id={"tp": dev}, device_id_type=MESH)
    pl.semaphore_wait(bar, 2)
    for q in range(4):
        for j in range(2):
            far_copy(q, j).start()
    for j in range(2):
        sib_copy(j).start()

    def block(blk, carry):
        odd = jnp.where(blk == 3, 1, 0)
        dodd = jnp.where(blk == 2, 1, 0)
        n_w = jnp.where(blk == 1, 8, jnp.where(blk == 2, 5, jnp.where(blk == 3, 1, 0)))

        def f_step(i, carry):
            t, n, slot = 2 * blk + i // 4, i % 4, (i + odd) % 2
            ls = (i // 4 + odd) % 2

            @pl.when((blk == 3) & (i == 3))
            def _():
                forward(3)

            @pl.when((blk == 3) & (i == 4))
            def _():
                for j in range(2):
                    fwd_copy(3, j).wait_recv()
                f_lhs(t, ls)
            pl.when(n == 0)(lambda: f_lhs_wait(ls))
            for c in f_rhs(n, slot):
                c.wait()

            @pl.when((i < 7) | (blk == 0))
            def _():
                for c in f_rhs((n + 1) % 4, 1 - slot):
                    c.start()

            @pl.when((n == 3) & ((i == 7) & (blk == 0) | (i == 3) & (blk < 3)))
            def _():
                @pl.when((blk == 0) & (i == 7))
                def _():
                    for j in range(2):
                        sib_copy(j).wait_recv()

                @pl.when(blk == 2)
                def _():
                    for j in range(2):
                        fwd_copy(1, j).wait_recv()
                f_lhs(t + 1, 1 - ls)

            @pl.when((i == 7) & (blk > 0))
            def _():
                unit, k = w_of(blk, 0)
                w_lhs(unit, k, odd)
                w_rhs(unit, k, odd)

            @pl.when((i >= 2) | (blk == 1))
            def _():
                for c in f_outs(t, n, slot):
                    c.wait()

            @pl.when((i < 2) & (blk == 2))
            def _():
                for h in range(2):
                    d_send_own(1, i, slot, h).wait_send()

            @pl.when((i < 2) & (blk == 3))
            def _():
                for h in range(2):
                    d_out(s01, i, slot, h).wait()
                pl.when(i == 1)(lambda: s_copy().start())

            _gate(la.at[ls], lb.at[ls], wn.at[slot], wt.at[slot, 0], ob.at[slot])
            for c in f_outs(t, n, slot):
                c.start()
            return carry

        lax.fori_loop(0, 8, f_step, 0)

        def w_step(grp, carry):
            unit, k = w_of(blk, grp)
            ls = (grp + odd) % 2
            last = jnp.where(unit < 4, 1, 2)

            @pl.when((blk == 1) & (grp == 0))
            def _():
                forward(0)

            @pl.when((blk == 2) & (grp == 1))
            def _():
                forward(2)
            w_lhs_wait(ls)
            w_rhs_wait(ls)

            @pl.when((grp == 0) & (blk != 2) | (grp == 1) & (blk == 2))
            def _():
                for s in range(2):
                    for c in f_outs(0, 0, s):
                        c.wait()

            @pl.when(grp + 1 < n_w)
            def _():
                unit2, k2 = w_of(blk, grp + 1)
                w_lhs(unit2, k2, 1 - ls)
                w_rhs(unit2, k2, 1 - ls)

            @pl.when(grp + 1 == n_w)
            def _():
                d_lhs(blk, 0, 1 - ls)
                for c in d_rhs(0, 1 - ls):
                    c.start()

            @pl.when((k == 0) & (unit > 0))
            def _():
                for n in range(2):
                    w_out_wait(n)
            _wgrad(acc, 0, la.at[ls], wn.at[ls], lb.at[ls], k > 0)
            pl.when(k == last)(lambda: w_out(unit))
            return carry

        lax.fori_loop(0, n_w, w_step, 0)

        def d_step(i, carry):
            g, n, slot = i // 2, i % 2, (i + dodd) % 2
            ls = (g + dodd) % 2
            mine = (blk > 1) & (g == 1)

            @pl.when((blk == 1) & (i == 1))
            def _():
                forward(1)
            pl.when(n == 0)(lambda: d_lhs_wait(ls))
            for c in d_rhs(n, slot):
                c.wait()

            @pl.when(mine)
            def _():
                for h in range(2):
                    d_send_far(blk, n, slot, h).wait_recv()

            @pl.when(i < 3)
            def _():
                for c in d_rhs(1 - n, 1 - slot):
                    c.start()
            pl.when(i == 0)(lambda: d_lhs(blk, 1, 1 - ls))

            @pl.when((i == 2) & (blk < 3))
            def _():
                @pl.when(blk == 1)
                def _():
                    for j in range(2):
                        fwd_copy(0, j).wait_recv()

                @pl.when(blk == 2)
                def _():
                    for j in range(2):
                        fwd_copy(2, j).wait_recv()
                f_lhs(2 * blk + 2, 1 - ls)

            @pl.when((i == 3) & (blk < 3))
            def _():
                for c in f_rhs(0, 1 - slot):
                    c.start()

            @pl.when(i >= 2)
            def _():
                for h in range(2):
                    d_send_own(0, n, slot, h).wait_send()

            p = [_dot(la[ls, :, pl.ds(0, T)], wn[slot, pl.ds(h * C, C)], NT)
                 + _dot(la[ls, :, pl.ds(T, T)], wn[slot, pl.ds(T + h * C, C)], NT) + _dot(lb[ls], wt[slot, h], NT) for h in range(2)]
            for h in range(2):
                ob[slot, h] = (p[h] + rcv[jnp.where(mine, 2 * n + h, 4)].astype(F32)).astype(BF16)
            for h in range(2):
                pl.when(blk == 1)(lambda: d_send_own(g, n, slot, h).start())
                pl.when((blk > 1) & (g == 0))(lambda: d_send_far(blk, n, slot, h).start())
                pl.when(mine & (blk == 2))(lambda: d_out(s01, n, slot, h).start())
                pl.when(mine & (blk == 3))(lambda: d_out(s23, n, slot, h).start())
            return carry

        @pl.when(blk > 0)
        def _():
            lax.fori_loop(0, 4, d_step, 0)
        return carry

    lax.fori_loop(0, 4, block, 0)

    for s in range(2):
        for h in range(2):
            d_out(s23, s, s, h).wait()
        w_out_wait(s)
    for j in range(2):
        sib_copy(j).wait_send()
        for q in range(4):
            far_copy(q, j).wait_send()
            fwd_copy(q, j).wait_send()
    for i in range(8):
        d_send_own(i // 4, i // 2 % 2, 0, i % 2).wait_recv()
    s_copy().wait()


def _k2(dya, xa, z, dug, duu, psib, r01, wg, wu, pg, pu, pd, dwg, dwu, dwd, dx,
        la, lb, wn, wt, ob, acc, add, lsem, rsem, osem, asem, psem, dsem):
    copy = pltpu.make_async_copy
    n_w = 10

    def w_of(grp):
        unit = jnp.where(grp < 8, grp // 2, grp - 4)
        k = jnp.where(grp < 8, 2 + grp % 2, 3)
        return unit, k

    def w_lhs(unit, k, slot):
        def go(src, row):
            for j in range(2):
                copy(src.at[_ds(2 * row + j, T), _ds(unit % 2, T)], la.at[slot, :, pl.ds(j * T, T)], lsem.at[slot, j]).start()
        pl.when(unit < 4)(lambda: go(xa, k - 1))
        pl.when(unit >= 4)(lambda: go(z, k))

    def w_rhs(unit, k, slot):
        def go(src, row):
            copy(src.at[_ds(row, S), pl.ds(0, T)], wn.at[slot], rsem.at[slot, 0]).start()
            for j in range(2):
                copy(src.at[_ds(2 * row + j, T), pl.ds(T, T)], lb.at[slot, :, pl.ds(j * T, T)], rsem.at[slot, 1 + j]).start()
        pl.when(unit < 2)(lambda: go(dug, k))
        pl.when((unit >= 2) & (unit < 4))(lambda: go(duu, k))
        pl.when(unit >= 4)(lambda: go(dya, k - 1))

    def w_wait(slot):
        copy(dug.at[pl.ds(0, S), pl.ds(0, T)], wn.at[slot], rsem.at[slot, 0]).wait()
        for j in range(2):
            copy(xa.at[pl.ds(0, T), pl.ds(0, T)], la.at[slot, :, pl.ds(j * T, T)], lsem.at[slot, j]).wait()
            copy(xa.at[pl.ds(0, T), pl.ds(0, T)], lb.at[slot, :, pl.ds(j * T, T)], rsem.at[slot, 1 + j]).wait()

    def w_part(unit):
        def go(src):
            for n in range(2):
                a = 2 * (unit % 2) + n
                copy(src.at[_ds(unit % 2, T), pl.ds(n * T, T)], acc.at[a], psem.at[a]).start()
        pl.when(unit < 2)(lambda: go(pg))
        pl.when((unit >= 2) & (unit < 4))(lambda: go(pu))
        pl.when(unit >= 4)(lambda: go(pd))

    def w_part_wait(unit):
        for n in range(2):
            a = 2 * (unit % 2) + n
            copy(pg.at[pl.ds(0, T), pl.ds(0, T)], acc.at[a], psem.at[a]).wait()

    def w_out(unit):
        def go(dst):
            for n in range(2):
                a = 2 * (unit % 2) + n
                copy(acc.at[a], dst.at[_ds(unit % 2, T), pl.ds(n * T, T)], asem.at[a]).start()
        pl.when(unit < 2)(lambda: go(dwg))
        pl.when((unit >= 2) & (unit < 4))(lambda: go(dwu))
        pl.when(unit >= 4)(lambda: go(dwd))

    def w_out_wait(unit):
        for n in range(2):
            a = 2 * (unit % 2) + n
            copy(acc.at[a], dwg.at[pl.ds(0, T), pl.ds(0, T)], asem.at[a]).wait()

    def d_lhs(slot):
        return (copy(dug.at[pl.ds(0, T)], la.at[slot], lsem.at[slot, 0]),
                copy(duu.at[pl.ds(0, T)], lb.at[slot], lsem.at[slot, 1]))

    def d_rhs(n, slot):
        return (copy(wg.at[_ds(n, C)], wt.at[slot, 0], rsem.at[slot, 0]),
                copy(wu.at[_ds(n, C)], wt.at[slot, 1], rsem.at[slot, 1]),
                copy(psib.at[pl.ds(0, T), _ds(n, C)], add.at[slot, 0], dsem.at[slot, 0]),
                copy(r01.at[:, _ds(n, C)], add.at[slot, 1], dsem.at[slot, 1]))

    def d_out(n, slot):
        return copy(ob.at[slot], dx.at[pl.ds(0, T), _ds(n, C)], osem.at[slot])

    w_lhs(0, 2, 0)
    w_rhs(0, 2, 0)
    w_part(0)

    def w_step(grp, carry):
        unit, k = w_of(grp)
        ls = grp % 2
        w_wait(ls)

        @pl.when(grp + 1 < n_w)
        def _():
            unit2, k2 = w_of(grp + 1)
            w_lhs(unit2, k2, 1 - ls)
            w_rhs(unit2, k2, 1 - ls)

        @pl.when(grp + 1 == n_w)
        def _():
            for c in (*d_lhs(0), *d_rhs(0, 0)):
                c.start()

        @pl.when((grp >= 8) | (k == 2))
        def _():
            w_part_wait(unit)

            @pl.when(unit < 5)
            def _():
                pl.when(unit > 0)(lambda: w_out_wait(unit + 1))
                w_part(unit + 1)
        _wgrad(acc, 2 * (unit % 2), la.at[ls], wn.at[ls], lb.at[ls], None)
        pl.when(k == 3)(lambda: w_out(unit))
        return carry

    lax.fori_loop(0, n_w, w_step, 0)

    def d_step(n, carry):
        slot = n % 2

        @pl.when(n == 0)
        def _():
            for c in d_lhs(0):
                c.wait()
        for c in d_rhs(n, slot):
            c.wait()

        @pl.when(n < 3)
        def _():
            for c in d_rhs(n + 1, 1 - slot):
                c.start()
        pl.when(n >= 2)(lambda: d_out(n, slot).wait())
        p = _dot(la[0], wt[slot, 0], NT) + _dot(lb[0], wt[slot, 1], NT)
        ob[slot] = (p + add[slot, 0].astype(F32) + add[slot, 1].astype(F32)).astype(BF16)
        d_out(n, slot).start()
        return carry

    lax.fori_loop(0, 4, d_step, 0)
    for s in range(2):
        d_out(2 + s, s).wait()
        w_out_wait(s)


def _k3(dug, duu, wg, wu, p1, p2, _, dx):
    p = _dot(dug[...], wg[...], NT) + _dot(duu[...], wu[...], NT)
    dx[...] = (p + p1[...].astype(F32) + p2[...].astype(F32)).astype(BF16)


def _local(x, dy, wg, wu, wd):
    def bf(r):
        return jax.ShapeDtypeStruct((r, S), BF16)

    def ff(r):
        return jax.ShapeDtypeStruct((r, S), F32)
    k1 = pl.pallas_call(
        _k1, name="gather_gate",
        out_shape=(bf(3 * S), bf(3 * S), bf(4 * S), bf(4 * S), bf(4 * S), bf(S), bf(T), bf(T), bf(T), ff(S), ff(S), ff(S)),
        in_specs=[ANY] * 5, out_specs=(ANY,) * 12,
        scratch_shapes=[pltpu.VMEM((2, T, S), BF16), pltpu.VMEM((2, T, S), BF16), pltpu.VMEM((2, S, T), BF16),
                        pltpu.VMEM((2, 2, C, S), BF16), pltpu.VMEM((2, 3, T, C), BF16), pltpu.VMEM((2, T, T), F32),
                        pltpu.VMEM((5, T, C), BF16), DMA((2, 4)), DMA((2, 4)), DMA((2, 3)), DMA((2,)),
                        DMA((8,)), DMA((8,)), DMA((2,)), DMA((2,)), DMA((8,)), DMA((8,)), DMA((2, 2)), DMA((16,)),
                        DMA((1,)), DMA((1,))],
        cost_estimate=pl.CostEstimate(flops=420_000_000_000, bytes_accessed=1 << 30, transcendentals=0),
        compiler_params=pltpu.CompilerParams(collective_id=0, has_side_effects=True, vmem_limit_bytes=VMEM))
    xa, dya, z, dug, duu, psib, _, s23, r01, pg, pu, pd = k1(x, dy, wg, wu, wd)
    r23 = lax.ppermute(s23, "tp", [(0, 2), (2, 0), (1, 3), (3, 1)])
    k2 = pl.pallas_call(
        _k2, name="wgrad_dx",
        out_shape=(ff(S), ff(S), ff(S), bf(S)),
        in_specs=[ANY] * 12, out_specs=(ANY,) * 4,
        scratch_shapes=[pltpu.VMEM((2, T, S), BF16), pltpu.VMEM((2, T, S), BF16), pltpu.VMEM((2, S, T), BF16),
                        pltpu.VMEM((2, 2, C, S), BF16), pltpu.VMEM((2, T, C), BF16), pltpu.VMEM((4, T, T), F32),
                        pltpu.VMEM((2, 2, T, C), BF16), DMA((2, 2)), DMA((2, 3)), DMA((2,)), DMA((4,)), DMA((4,)), DMA((2, 2))],
        cost_estimate=pl.CostEstimate(flops=105_000_000_000, bytes_accessed=1 << 28, transcendentals=0),
        compiler_params=pltpu.CompilerParams(vmem_limit_bytes=VMEM))
    dwg, dwu, dwd, dx = k2(dya, xa, z, dug, duu, psib, r01, wg, wu, pg, pu, pd)
    row = pl.BlockSpec((T, S), lambda n: (1, 0))
    col = pl.BlockSpec((C, S), lambda n: (n, 0))
    tile = pl.BlockSpec((T, C), lambda n: (1, n))
    dx = pl.pallas_call(
        _k3, name="dx", out_shape=bf(S), grid=(S // C,),
        in_specs=[row, row, col, col, tile, pl.BlockSpec((T, C), lambda n: (0, n)), ANY],
        out_specs=tile, input_output_aliases={6: 0},
        cost_estimate=pl.CostEstimate(flops=4 * T * S * S, bytes_accessed=1 << 25, transcendentals=0),
        compiler_params=pltpu.CompilerParams(vmem_limit_bytes=60 << 20))(dug, duu, wg, wu, psib, r23, dx)
    return dx, dwg, dwu, dwd


def solution(mesh):
    rows = P(("dp", "tp"), None)
    return jax.shard_map(_local, mesh=mesh,
                         in_specs=(rows, rows, P(None, "tp"), P(None, "tp"), P("tp", None)),
                         out_specs=(rows, P("dp", "tp"), P("dp", "tp"), rows),
                         check_vma=False)
```

```python
import jax
import jax.numpy as jnp
from jax import lax
from jax.experimental import pallas as pl
from jax.experimental.pallas import tpu as pltpu
from jax.sharding import PartitionSpec as P

F32, BF16 = jnp.float32, jnp.bfloat16
NN = (((1,), (0,)), ((), ()))
NT = (((1,), (1,)), ((), ()))
TN = (((0,), (0,)), ((), ()))
ANY = pl.BlockSpec(memory_space=pl.ANY)
MESH = pl.DeviceIdType.MESH
DMA = pltpu.SemaphoreType.DMA

S = 2048
T = 1024
C = 512
P8 = 256
VMEM = 67043328


def _dot(a, b, dims):
    return lax.dot_general(a, b, dims, preferred_element_type=F32)


def _ds(i, n):
    return pl.ds(pl.multiple_of(i * n, n), n)


def _gate(la, lb, wn, wt, ob):
    g = _dot(lb[...], wt[...], NT)
    ug = _dot(la[...], wn[:, pl.ds(0, C)], NN).astype(BF16).astype(F32)
    s = jax.nn.sigmoid(ug)
    a = ug * s
    ob[2] = (g * a).astype(BF16)
    gd = g * (s * (1.0 + ug * (1.0 - s)))
    uu = _dot(la[...], wn[:, pl.ds(C, C)], NN).astype(BF16).astype(F32)
    ob[0] = (a * uu).astype(BF16)
    ob[1] = (gd * uu).astype(BF16)


def _wgrad(acc, base, la, wn, lb, keep):
    a0, a1 = la[:, pl.ds(0, T)], la[:, pl.ds(T, T)]
    rhs = ((wn[pl.ds(0, T), :], wn[pl.ds(T, T), :]), (lb[:, pl.ds(0, T)], lb[:, pl.ds(T, T)]))
    for n in range(2):
        old = acc[base + n]
        old = old if keep is None else jnp.where(keep, old, 0.0)
        acc[base + n] = old + _dot(a0, rhs[n][0], TN) + _dot(a1, rhs[n][1], TN)


def _k1(x, dy, wg, wu, wd, xa, dya, z, dug, duu, psib, s01, s23, r01, pg, pu, pd,
        la, lb, wn, wt, ob, acc, rcv, lsem, rsem, osem, asem,
        far_s, far_r, sib_s, sib_r, fwd_s, fwd_r, p_s, p_r, s_s, s_r):
    me = lax.axis_index("tp")
    sib = me // 2 * 2 + 1 - me % 2
    far = (me + 2) % 4
    copy = pltpu.make_async_copy

    def remote(src, dst, ss, rs, dev):
        return pltpu.make_async_remote_copy(src_ref=src, dst_ref=dst, send_sem=ss, recv_sem=rs,
                                            device_id={"tp": dev}, device_id_type=MESH)

    def far_copy(q, j):
        src, dst = ((x, xa), (dy, dya))[j]
        return remote(src.at[pl.ds(q * C, C)], dst.at[pl.ds(S + q * T, C)], far_s.at[2 * q + j], far_r.at[2 * q + j], far)

    def sib_copy(i, j):
        src, dst = ((x, xa), (dy, dya))[j]
        return remote(src.at[_ds(i, P8)], dst.at[_ds(i, P8)], sib_s.at[2 * i + j], sib_r.at[2 * i + j], sib)

    def fwd_copy(q, j):
        buf = (xa, dya)[j]
        return remote(buf.at[pl.ds(S + q * T, C)], buf.at[pl.ds(S + q * T + C, C)], fwd_s.at[2 * q + j], fwd_r.at[2 * q + j], sib)

    def forward(q, j):
        far_copy(q, j).wait_recv()
        fwd_copy(q, j).start()

    def s_copy():
        return remote(s01, r01, s_s.at[0], s_r.at[0], far)

    def f_lhs(t, slot):
        def go(a, b, row):
            copy(a.at[_ds(row, T)], la.at[slot], lsem.at[slot, 0]).start()
            copy(b.at[_ds(row, T)], lb.at[slot], lsem.at[slot, 1]).start()
        pl.when(t < 2)(lambda: go(x, dy, t))
        pl.when(t >= 2)(lambda: go(xa, dya, t - 2))

    def f_lhs_wait(slot):
        copy(x.at[pl.ds(0, T)], la.at[slot], lsem.at[slot, 0]).wait()
        copy(dy.at[pl.ds(0, T)], lb.at[slot], lsem.at[slot, 1]).wait()

    def f_rhs(n, slot):
        return (copy(wg.at[:, _ds(n, C)], wn.at[slot, :, pl.ds(0, C)], rsem.at[slot, 0]),
                copy(wu.at[:, _ds(n, C)], wn.at[slot, :, pl.ds(C, C)], rsem.at[slot, 1]),
                copy(wd.at[_ds(n, C)], wt.at[slot, 0], rsem.at[slot, 2]))

    def f_outs(t, n, slot):
        return [copy(ob.at[slot, j], dst.at[_ds(t, T), _ds(n, C)], osem.at[slot, j]) for j, dst in enumerate((z, dug, duu))]

    def d_lhs(blk, g, slot):
        for j in range(2):
            row = jnp.where(blk == 1, 4 + 2 * g + j, 8 + 2 * (2 * (blk - 2) + j) + 1 - g)
            copy(dug.at[_ds(row, C)], la.at[slot, pl.ds(j * C, C)], lsem.at[slot, 2 * j]).start()
            copy(duu.at[_ds(row, C)], lb.at[slot, pl.ds(j * C, C)], lsem.at[slot, 2 * j + 1]).start()

    def d_lhs_wait(slot):
        for j in range(2):
            copy(dug.at[pl.ds(0, C)], la.at[slot, pl.ds(j * C, C)], lsem.at[slot, 2 * j]).wait()
            copy(duu.at[pl.ds(0, C)], lb.at[slot, pl.ds(j * C, C)], lsem.at[slot, 2 * j + 1]).wait()

    def d_rhs(n, slot):
        return [copy(wg.at[_ds(n, T), pl.ds(j * T, T)], wn.at[slot, pl.ds(j * T, T)], rsem.at[slot, j]) for j in range(2)] + [
            copy(wu.at[_ds(2 * n + j, C)], wt.at[slot, j], rsem.at[slot, 2 + j]) for j in range(2)]

    def d_send_own(g, n, slot, h):
        return remote(ob.at[slot, h], psib.at[_ds(g, T), _ds(2 * n + h, C)], p_s.at[slot, h], p_r.at[4 * g + 2 * n + h], sib)

    def d_send_far(blk, n, slot, h):
        return remote(ob.at[slot, h], rcv.at[2 * n + h], p_s.at[slot, h], p_r.at[4 * blk + 2 * n + h], sib)

    def d_out(dst, n, slot, h):
        return copy(ob.at[slot, h], dst.at[:, _ds(2 * n + h, C)], osem.at[slot, h])

    def w_of(blk, grp):
        h = jnp.where(blk == 3, 5, grp)
        unit = jnp.where(blk == 1, grp // 2, 4 + h // 3)
        k = jnp.where(blk == 1, grp % 2, h % 3)
        return unit, k

    def w_lhs(unit, k, slot):
        m = unit % 2

        def go(src, row):
            for j in range(2):
                copy(src.at[_ds(2 * row + j, T), _ds(m, T)], la.at[slot, :, pl.ds(j * T, T)], lsem.at[slot, j]).start()
        pl.when((unit < 4) & (k == 0))(lambda: go(x, 0))
        pl.when((unit < 4) & (k > 0))(lambda: go(xa, k - 1))
        pl.when(unit >= 4)(lambda: go(z, k))

    def w_lhs_wait(slot):
        for j in range(2):
            copy(x.at[pl.ds(0, T), pl.ds(0, T)], la.at[slot, :, pl.ds(j * T, T)], lsem.at[slot, j]).wait()

    def w_rhs(unit, k, slot):
        def go(src, row):
            copy(src.at[_ds(row, S), pl.ds(0, T)], wn.at[slot], rsem.at[slot, 0]).start()
            for j in range(2):
                copy(src.at[_ds(2 * row + j, T), pl.ds(T, T)], lb.at[slot, :, pl.ds(j * T, T)], rsem.at[slot, 1 + j]).start()
        pl.when(unit < 2)(lambda: go(dug, k))
        pl.when((unit >= 2) & (unit < 4))(lambda: go(duu, k))
        pl.when((unit >= 4) & (k == 0))(lambda: go(dy, 0))
        pl.when((unit >= 4) & (k > 0))(lambda: go(dya, k - 1))

    def w_rhs_wait(slot):
        copy(x.at[:, pl.ds(0, T)], wn.at[slot], rsem.at[slot, 0]).wait()
        for j in range(2):
            copy(x.at[pl.ds(0, T), pl.ds(0, T)], lb.at[slot, :, pl.ds(j * T, T)], rsem.at[slot, 1 + j]).wait()

    def w_out(unit):
        def go(dst):
            for n in range(2):
                copy(acc.at[n], dst.at[_ds(unit % 2, T), pl.ds(n * T, T)], asem.at[n]).start()
        pl.when(unit < 2)(lambda: go(pg))
        pl.when((unit >= 2) & (unit < 4))(lambda: go(pu))
        pl.when(unit >= 4)(lambda: go(pd))

    def w_out_wait(n):
        copy(acc.at[n], pg.at[pl.ds(0, T), pl.ds(0, T)], asem.at[n]).wait()

    f_lhs(0, 0)
    for c in f_rhs(0, 0):
        c.start()
    rcv[4] = jnp.zeros_like(rcv[4])
    bar = pltpu.get_barrier_semaphore()
    for dev in (sib, far):
        pl.semaphore_signal(bar, inc=1, device_id={"tp": dev}, device_id_type=MESH)
    pl.semaphore_wait(bar, 2)
    for q in range(4):
        for j in range(2):
            far_copy(q, j).start()

    def block(blk, carry):
        odd = jnp.where(blk == 3, 1, 0)
        dodd = jnp.where(blk == 2, 1, 0)
        n_w = jnp.where(blk == 1, 8, jnp.where(blk == 2, 5, jnp.where(blk == 3, 1, 0)))

        def f_step(i, carry):
            t, n, slot = 2 * blk + i // 4, i % 4, (i + odd) % 2
            ls = (i // 4 + odd) % 2

            @pl.when(blk == 3)
            def _():
                pl.when(i == 1)(lambda: forward(3, 0))
                pl.when(i == 2)(lambda: forward(3, 1))
            pl.when(n == 0)(lambda: f_lhs_wait(ls))
            for c in f_rhs(n, slot):
                c.wait()

            @pl.when((i < 7) | (blk == 0))
            def _():
                for c in f_rhs((n + 1) % 4, 1 - slot):
                    c.start()

            @pl.when((i == 7) & (blk == 0) | (i == 3))
            def _():
                @pl.when((t == 1) | (t == 2))
                def _():
                    for j in range(8):
                        sib_copy(4 * (t - 1) + j // 2, j % 2).wait_recv()

                @pl.when(blk > 1)
                def _():
                    for j in range(2):
                        fwd_copy(2 * blk - 3, j).wait_recv()
                f_lhs(t + 1, 1 - ls)

            @pl.when((i == 7) & (blk > 0))
            def _():
                unit, k = w_of(blk, 0)
                w_lhs(unit, k, odd)
                w_rhs(unit, k, odd)

            @pl.when(blk == 0)
            def _():
                for j in range(2):
                    sib_copy(i, j).start()

            @pl.when((i >= 2) | (blk == 1))
            def _():
                for c in f_outs(t, n, slot):
                    c.wait()

            @pl.when((i < 2) & (blk == 2))
            def _():
                for h in range(2):
                    d_send_own(1, i, slot, h).wait_send()

            @pl.when((i < 2) & (blk == 3))
            def _():
                for h in range(2):
                    d_out(s01, i, slot, h).wait()
                pl.when(i == 1)(lambda: s_copy().start())

            _gate(la.at[ls], lb.at[ls], wn.at[slot], wt.at[slot, 0], ob.at[slot])
            for c in f_outs(t, n, slot):
                c.start()
            return carry

        lax.fori_loop(0, 8, f_step, 0)

        def w_step(grp, carry):
            unit, k = w_of(blk, grp)
            ls = (grp + odd) % 2
            last = jnp.where(unit < 4, 1, 2)

            w_lhs_wait(ls)
            w_rhs_wait(ls)

            @pl.when((grp == 0) & (blk != 2) | (grp == 1) & (blk == 2))
            def _():
                for s in range(2):
                    for c in f_outs(0, 0, s):
                        c.wait()

            @pl.when(grp + 1 < n_w)
            def _():
                unit2, k2 = w_of(blk, grp + 1)
                w_lhs(unit2, k2, 1 - ls)
                w_rhs(unit2, k2, 1 - ls)

            @pl.when(grp + 1 == n_w)
            def _():
                d_lhs(blk, 0, 1 - ls)
                for c in d_rhs(0, 1 - ls):
                    c.start()

            for j in range(2):
                pl.when((blk == 1) & (grp == j))(lambda: forward(0, j))
                pl.when((blk == 2) & (grp == 1 + j))(lambda: forward(2, j))

            @pl.when((k == 0) & (unit > 0))
            def _():
                for n in range(2):
                    w_out_wait(n)
            _wgrad(acc, 0, la.at[ls], wn.at[ls], lb.at[ls], k > 0)
            pl.when(k == last)(lambda: w_out(unit))
            return carry

        lax.fori_loop(0, n_w, w_step, 0)

        def d_step(i, carry):
            g, n, slot = i // 2, i % 2, (i + dodd) % 2
            ls = (g + dodd) % 2
            mine = (blk > 1) & (g == 1)

            pl.when(n == 0)(lambda: d_lhs_wait(ls))
            for c in d_rhs(n, slot):
                c.wait()

            @pl.when(mine)
            def _():
                for h in range(2):
                    d_send_far(blk, n, slot, h).wait_recv()

            @pl.when(i < 3)
            def _():
                for c in d_rhs(1 - n, 1 - slot):
                    c.start()
            pl.when(i == 0)(lambda: d_lhs(blk, 1, 1 - ls))

            @pl.when((i == 2) & (blk < 3))
            def _():
                @pl.when(blk == 1)
                def _():
                    for j in range(2):
                        fwd_copy(0, j).wait_recv()

                @pl.when(blk == 2)
                def _():
                    for j in range(2):
                        fwd_copy(2, j).wait_recv()
                f_lhs(2 * blk + 2, 1 - ls)

            @pl.when((i == 3) & (blk < 3))
            def _():
                for c in f_rhs(0, 1 - slot):
                    c.start()

            for j in range(2):
                pl.when((blk == 1) & (i == 1 + j))(lambda: forward(1, j))

            @pl.when(i >= 2)
            def _():
                for h in range(2):
                    d_send_own(0, n, slot, h).wait_send()

            p = [_dot(la[ls, :, pl.ds(0, T)], wn[slot, pl.ds(h * C, C)], NT)
                 + _dot(la[ls, :, pl.ds(T, T)], wn[slot, pl.ds(T + h * C, C)], NT) + _dot(lb[ls], wt[slot, h], NT) for h in range(2)]
            for h in range(2):
                ob[slot, h] = (p[h] + rcv[jnp.where(mine, 2 * n + h, 4)].astype(F32)).astype(BF16)
            for h in range(2):
                pl.when(blk == 1)(lambda: d_send_own(g, n, slot, h).start())
                pl.when((blk > 1) & (g == 0))(lambda: d_send_far(blk, n, slot, h).start())
                pl.when(mine & (blk == 2))(lambda: d_out(s01, n, slot, h).start())
                pl.when(mine & (blk == 3))(lambda: d_out(s23, n, slot, h).start())
            return carry

        @pl.when(blk > 0)
        def _():
            lax.fori_loop(0, 4, d_step, 0)
        return carry

    lax.fori_loop(0, 4, block, 0)

    for s in range(2):
        for h in range(2):
            d_out(s23, s, s, h).wait()
        w_out_wait(s)
    for i in range(8):
        for j in range(2):
            sib_copy(i, j).wait_send()
    for q in range(4):
        for j in range(2):
            far_copy(q, j).wait_send()
            fwd_copy(q, j).wait_send()
    for i in range(8):
        d_send_own(i // 4, i // 2 % 2, 0, i % 2).wait_recv()
    s_copy().wait()


def _k2(dya, xa, z, dug, duu, psib, r01, wg, wu, pg, pu, pd, dwg, dwu, dwd, dx,
        la, lb, wn, ob, acc, add, lsem, rsem, osem, asem, psem, dsem):
    copy = pltpu.make_async_copy
    n_w = 10

    def w_of(grp):
        pos = sum(jnp.where(grp >= g, 1, 0) for g in (2, 3, 5, 7, 8))
        k = 3 - sum(jnp.where(grp == g, 1, 0) for g in (0, 3, 5, 8))
        return unit_of(pos), pos, k

    def unit_of(pos):
        return jnp.where(pos == 1, 4, jnp.where(pos == 4, 5, pos - jnp.where(pos > 4, 2, jnp.where(pos > 1, 1, 0))))

    def w_lhs(unit, k, slot):
        def go(src, row):
            for j in range(2):
                copy(src.at[_ds(2 * row + j, T), _ds(unit % 2, T)], la.at[slot, :, pl.ds(j * T, T)], lsem.at[slot, j]).start()
        pl.when(unit < 4)(lambda: go(xa, k - 1))
        pl.when(unit >= 4)(lambda: go(z, k))

    def w_rhs(unit, k, slot):
        def go(src, row):
            copy(src.at[_ds(row, S), pl.ds(0, T)], wn.at[slot], rsem.at[slot, 0]).start()
            for j in range(2):
                copy(src.at[_ds(2 * row + j, T), pl.ds(T, T)], lb.at[slot, :, pl.ds(j * T, T)], rsem.at[slot, 1 + j]).start()
        pl.when(unit < 2)(lambda: go(dug, k))
        pl.when((unit >= 2) & (unit < 4))(lambda: go(duu, k))
        pl.when(unit >= 4)(lambda: go(dya, k - 1))

    def w_wait(slot):
        copy(dug.at[pl.ds(0, S), pl.ds(0, T)], wn.at[slot], rsem.at[slot, 0]).wait()
        for j in range(2):
            copy(xa.at[pl.ds(0, T), pl.ds(0, T)], la.at[slot, :, pl.ds(j * T, T)], lsem.at[slot, j]).wait()
            copy(xa.at[pl.ds(0, T), pl.ds(0, T)], lb.at[slot, :, pl.ds(j * T, T)], rsem.at[slot, 1 + j]).wait()

    def w_tile(unit, n):
        return _ds(unit % 2, T), pl.ds(n * T, T)

    def w_part(pos):
        unit = unit_of(pos)

        def go(src):
            for n in range(2):
                a = 2 * (pos % 3) + n
                copy(src.at[w_tile(unit, n)], acc.at[a], psem.at[a]).start()
        pl.when(unit < 2)(lambda: go(pg))
        pl.when((unit >= 2) & (unit < 4))(lambda: go(pu))
        pl.when(unit >= 4)(lambda: go(pd))

    def w_part_wait(pos):
        for n in range(2):
            a = 2 * (pos % 3) + n
            copy(pg.at[w_tile(0, n)], acc.at[a], psem.at[a]).wait()

    def w_out(pos):
        unit = unit_of(pos)

        def go(dst):
            for n in range(2):
                a = 2 * (pos % 3) + n
                copy(acc.at[a], dst.at[w_tile(unit, n)], asem.at[a]).start()
        pl.when(unit < 2)(lambda: go(dwg))
        pl.when((unit >= 2) & (unit < 4))(lambda: go(dwu))
        pl.when(unit >= 4)(lambda: go(dwd))

    def w_out_wait(pos):
        for n in range(2):
            a = 2 * (pos % 3) + n
            copy(acc.at[a], dwg.at[w_tile(0, n)], asem.at[a]).wait()

    def d_lhs(slot):
        return (copy(dug.at[pl.ds(0, T)], la.at[slot], lsem.at[slot, 0]),
                copy(duu.at[pl.ds(0, T)], lb.at[slot], lsem.at[slot, 1]))

    def d_rhs(n, slot):
        return [copy(w.at[_ds(n, C), pl.ds(j * T, T)], wn.at[slot, pl.ds((2 * k + j) * C, C)], rsem.at[slot, 2 * k + j])
                for k, w in enumerate((wg, wu)) for j in range(2)] + [
            copy(psib.at[pl.ds(0, T), _ds(n, C)], add.at[slot, 0], dsem.at[slot, 0]),
            copy(r01.at[:, _ds(n, C)], add.at[slot, 1], dsem.at[slot, 1])]

    def d_out(n, slot):
        return copy(ob.at[slot], dx.at[pl.ds(0, T), _ds(n, C)], osem.at[slot])

    w_lhs(0, 2, 0)
    w_rhs(0, 2, 0)
    w_part(0)

    def w_step(grp, carry):
        unit, pos, k = w_of(grp)
        ls = grp % 2
        w_wait(ls)

        @pl.when(grp + 1 < n_w)
        def _():
            unit2, _, k2 = w_of(grp + 1)
            w_lhs(unit2, k2, 1 - ls)
            w_rhs(unit2, k2, 1 - ls)

        @pl.when(grp + 1 == n_w)
        def _():
            for c in (*d_lhs(0), *d_rhs(0, 0)):
                c.start()

        @pl.when((k == 2) | (unit >= 4))
        def _():
            w_part_wait(pos)

            @pl.when(pos < 5)
            def _():
                pl.when(pos > 1)(lambda: w_out_wait(pos + 1))
                w_part(pos + 1)
        _wgrad(acc, 2 * (pos % 3), la.at[ls], wn.at[ls], lb.at[ls], None)
        pl.when(k == 3)(lambda: w_out(pos))
        return carry

    lax.fori_loop(0, n_w, w_step, 0)

    def d_step(n, carry):
        slot = n % 2

        @pl.when(n == 0)
        def _():
            for c in d_lhs(0):
                c.wait()
        for c in d_rhs(n, slot):
            c.wait()

        @pl.when(n < 3)
        def _():
            for c in d_rhs(n + 1, 1 - slot):
                c.start()
        pl.when(n >= 2)(lambda: d_out(n, slot).wait())
        p = sum(_dot(lhs[0, :, pl.ds(j * T, T)], wn[slot, pl.ds((2 * k + j) * C, C)], NT)
                for k, lhs in enumerate((la, lb)) for j in range(2))
        ob[slot] = (p + add[slot, 0].astype(F32) + add[slot, 1].astype(F32)).astype(BF16)
        d_out(n, slot).start()
        return carry

    lax.fori_loop(0, 4, d_step, 0)
    for s in range(2):
        d_out(2 + s, s).wait()
    for pos in range(3):
        w_out_wait(pos)


def _k3(dug, duu, wg, wu, p1, p2, _, dx):
    p = _dot(dug[...], wg[...], NT) + _dot(duu[...], wu[...], NT)
    dx[...] = (p + p1[...].astype(F32) + p2[...].astype(F32)).astype(BF16)


def _local(x, dy, wg, wu, wd):
    def bf(r):
        return jax.ShapeDtypeStruct((r, S), BF16)

    def ff(r):
        return jax.ShapeDtypeStruct((r, S), F32)
    k1 = pl.pallas_call(
        _k1, name="gather_gate",
        out_shape=(bf(3 * S), bf(3 * S), bf(4 * S), bf(4 * S), bf(4 * S), bf(S), bf(T), bf(T), bf(T), ff(S), ff(S), ff(S)),
        in_specs=[ANY] * 5, out_specs=(ANY,) * 12,
        scratch_shapes=[pltpu.VMEM((2, T, S), BF16), pltpu.VMEM((2, T, S), BF16), pltpu.VMEM((2, S, T), BF16),
                        pltpu.VMEM((2, 2, C, S), BF16), pltpu.VMEM((2, 3, T, C), BF16), pltpu.VMEM((2, T, T), F32),
                        pltpu.VMEM((5, T, C), BF16), DMA((2, 4)), DMA((2, 4)), DMA((2, 3)), DMA((2,)),
                        DMA((8,)), DMA((8,)), DMA((16,)), DMA((16,)), DMA((8,)), DMA((8,)), DMA((2, 2)), DMA((16,)),
                        DMA((1,)), DMA((1,))],
        cost_estimate=pl.CostEstimate(flops=420_000_000_000, bytes_accessed=1 << 30, transcendentals=0),
        compiler_params=pltpu.CompilerParams(collective_id=0, has_side_effects=True, vmem_limit_bytes=VMEM))
    xa, dya, z, dug, duu, psib, _, s23, r01, pg, pu, pd = k1(x, dy, wg, wu, wd)
    r23 = lax.ppermute(s23, "tp", [(0, 2), (2, 0), (1, 3), (3, 1)])
    k2 = pl.pallas_call(
        _k2, name="wgrad_dx",
        out_shape=(ff(S), ff(S), ff(S), bf(S)),
        in_specs=[ANY] * 12, out_specs=(ANY,) * 4,
        scratch_shapes=[pltpu.VMEM((2, T, S), BF16), pltpu.VMEM((2, T, S), BF16), pltpu.VMEM((2, S, T), BF16),
                        pltpu.VMEM((2, T, C), BF16), pltpu.VMEM((6, T, T), F32),
                        pltpu.VMEM((2, 2, T, C), BF16), DMA((2, 2)), DMA((2, 4)), DMA((2,)), DMA((6,)), DMA((6,)), DMA((2, 2))],
        cost_estimate=pl.CostEstimate(flops=105_000_000_000, bytes_accessed=1 << 28, transcendentals=0),
        compiler_params=pltpu.CompilerParams(vmem_limit_bytes=VMEM))
    dwg, dwu, dwd, dx = k2(dya, xa, z, dug, duu, psib, r01, wg, wu, pg, pu, pd)
    row = pl.BlockSpec((T, S), lambda n: (1, 0))
    col = pl.BlockSpec((C, S), lambda n: (n, 0))
    tile = pl.BlockSpec((T, C), lambda n: (1, n))
    dx = pl.pallas_call(
        _k3, name="dx", out_shape=bf(S), grid=(S // C,),
        in_specs=[row, row, col, col, tile, pl.BlockSpec((T, C), lambda n: (0, n)), ANY],
        out_specs=tile, input_output_aliases={6: 0},
        cost_estimate=pl.CostEstimate(flops=4 * T * S * S, bytes_accessed=1 << 25, transcendentals=0),
        compiler_params=pltpu.CompilerParams(vmem_limit_bytes=60 << 20))(dug, duu, wg, wu, psib, r23, dx)
    return dx, dwg, dwu, dwd


def solution(mesh):
    rows = P(("dp", "tp"), None)
    return jax.shard_map(_local, mesh=mesh,
                         in_specs=(rows, rows, P(None, "tp"), P(None, "tp"), P("tp", None)),
                         out_specs=(rows, P("dp", "tp"), P("dp", "tp"), rows),
                         check_vma=False)
```

```python
import jax
import jax.numpy as jnp
from jax import lax
from jax.experimental import pallas as pl
from jax.experimental.pallas import tpu as pltpu
from jax.sharding import PartitionSpec as P

F32, BF16 = jnp.float32, jnp.bfloat16
NN = (((1,), (0,)), ((), ()))
NT = (((1,), (1,)), ((), ()))
TN = (((0,), (0,)), ((), ()))
ANY = pl.BlockSpec(memory_space=pl.ANY)
MESH = pl.DeviceIdType.MESH
DMA = pltpu.SemaphoreType.DMA

S = 2048
T = 1024
C = 512
P8 = 256
VMEM = 67043328


def _dot(a, b, dims):
    return lax.dot_general(a, b, dims, preferred_element_type=F32)


def _ds(i, n):
    return pl.ds(pl.multiple_of(i * n, n), n)


def _gate(la, lb, wn, wt, ob):
    g = _dot(lb[...], wt[...], NT)
    ug = _dot(la[...], wn[:, pl.ds(0, C)], NN).astype(BF16).astype(F32)
    s = jax.nn.sigmoid(ug)
    a = ug * s
    ob[2] = (g * a).astype(BF16)
    gd = g * (s * (1.0 + ug * (1.0 - s)))
    uu = _dot(la[...], wn[:, pl.ds(C, C)], NN).astype(BF16).astype(F32)
    ob[0] = (a * uu).astype(BF16)
    ob[1] = (gd * uu).astype(BF16)


def _wgrad(acc, base, la, wn, lb, keep):
    a0, a1 = la[:, pl.ds(0, T)], la[:, pl.ds(T, T)]
    rhs = ((wn[pl.ds(0, T), :], wn[pl.ds(T, T), :]), (lb[:, pl.ds(0, T)], lb[:, pl.ds(T, T)]))
    for n in range(2):
        old = acc[base + n]
        old = old if keep is None else jnp.where(keep, old, 0.0)
        acc[base + n] = old + _dot(a0, rhs[n][0], TN) + _dot(a1, rhs[n][1], TN)


def half_of(unit):
    return jnp.where((unit == 2) | (unit >= 4), 1, 0)


def is_d(unit):
    return (unit == 0) | (unit == 5)


def is_g(unit):
    return (unit == 1) | (unit == 2)


def is_u(unit):
    return (unit == 3) | (unit == 4)


def _k1(x, dy, wg, wu, wd, xa, dya, z, dug, duu, psib, s01, s23, r01, pg, pu, pd,
        la, lb, wn, wt, ob, acc, rcv, lsem, rsem, osem, asem,
        far_s, far_r, sib_s, sib_r, fwd_s, fwd_r, p_s, p_r, s_s, s_r):
    me = lax.axis_index("tp")
    sib = me // 2 * 2 + 1 - me % 2
    far = (me + 2) % 4
    copy = pltpu.make_async_copy

    def remote(src, dst, ss, rs, dev):
        return pltpu.make_async_remote_copy(src_ref=src, dst_ref=dst, send_sem=ss, recv_sem=rs,
                                            device_id={"tp": dev}, device_id_type=MESH)

    def far_copy(q, j):
        src, dst = ((x, xa), (dy, dya))[j]
        return remote(src.at[pl.ds(q * C, C)], dst.at[pl.ds(S + q * T, C)], far_s.at[2 * q + j], far_r.at[2 * q + j], far)

    def sib_copy(i, j):
        src, dst = ((x, xa), (dy, dya))[j]
        return remote(src.at[_ds(i, P8)], dst.at[_ds(i, P8)], sib_s.at[2 * i + j], sib_r.at[2 * i + j], sib)

    def fwd_copy(q, j):
        buf = (xa, dya)[j]
        return remote(buf.at[_ds(4 + 2 * q, C)], buf.at[_ds(5 + 2 * q, C)], fwd_s.at[2 * q + j], fwd_r.at[2 * q + j], sib)

    def forward(q, j):
        far_copy(q, j).wait_recv()
        fwd_copy(q, j).start()

    def s_copy():
        return remote(s01, r01, s_s.at[0], s_r.at[0], far)

    def f_lhs(t, slot, j):
        own, all_, buf = ((x, xa, la), (dy, dya, lb))[j]

        @pl.when((t == 2) | (t == 3))
        def _():
            for i in range(4):
                sib_copy(4 * (t - 2) + i, j).wait_recv()
        pl.when(t >= 4)(lambda: fwd_copy(t - 4, j).wait_recv())
        pl.when(t < 2)(lambda: copy(own.at[_ds(t, T)], buf.at[slot], lsem.at[slot, j]).start())
        pl.when(t >= 2)(lambda: copy(all_.at[_ds(t - 2, T)], buf.at[slot], lsem.at[slot, j]).start())

    def f_lhs_wait(slot):
        copy(x.at[pl.ds(0, T)], la.at[slot], lsem.at[slot, 0]).wait()
        copy(dy.at[pl.ds(0, T)], lb.at[slot], lsem.at[slot, 1]).wait()

    def f_rhs(n, slot):
        return (copy(wg.at[:, _ds(n, C)], wn.at[slot, :, pl.ds(0, C)], rsem.at[slot, 0]),
                copy(wu.at[:, _ds(n, C)], wn.at[slot, :, pl.ds(C, C)], rsem.at[slot, 1]),
                copy(wd.at[_ds(n, C)], wt.at[slot, 0], rsem.at[slot, 2]))

    def f_outs(t, n, slot):
        return [copy(ob.at[slot, j], dst.at[_ds(t, T), _ds(n, C)], osem.at[slot, j]) for j, dst in enumerate((z, dug, duu))]

    def d_lhs(blk, g, slot):
        for j in range(2):
            row = jnp.where(blk == 1, 4 + 2 * g + j, 8 + 2 * (2 * (blk - 2) + j) + 1 - g)
            copy(dug.at[_ds(row, C)], la.at[slot, pl.ds(j * C, C)], lsem.at[slot, 2 * j]).start()
            copy(duu.at[_ds(row, C)], lb.at[slot, pl.ds(j * C, C)], lsem.at[slot, 2 * j + 1]).start()

    def d_lhs_wait(slot):
        for j in range(2):
            copy(dug.at[pl.ds(0, C)], la.at[slot, pl.ds(j * C, C)], lsem.at[slot, 2 * j]).wait()
            copy(duu.at[pl.ds(0, C)], lb.at[slot, pl.ds(j * C, C)], lsem.at[slot, 2 * j + 1]).wait()

    def d_rhs(n, slot):
        return [copy(wg.at[_ds(n, T), pl.ds(j * T, T)], wn.at[slot, pl.ds(j * T, T)], rsem.at[slot, j]) for j in range(2)] + [
            copy(wu.at[_ds(2 * n + j, C)], wt.at[slot, j], rsem.at[slot, 2 + j]) for j in range(2)]

    def d_send_own(g, n, slot, h):
        return remote(ob.at[slot, h], psib.at[_ds(g, T), _ds(2 * n + h, C)], p_s.at[slot, h], p_r.at[4 * g + 2 * n + h], sib)

    def d_send_far(blk, n, slot, h):
        return remote(ob.at[slot, h], rcv.at[2 * n + h], p_s.at[slot, h], p_r.at[4 * blk + 2 * n + h], sib)

    def d_out(dst, n, slot, h):
        return copy(ob.at[slot, h], dst.at[:, _ds(2 * n + h, C)], osem.at[slot, h])

    def w_of(blk, grp):
        h = jnp.where(blk == 3, 5, grp)
        unit = jnp.where(blk == 1, grp // 2, 4 + h // 3)
        k = jnp.where(blk == 1, grp % 2, h % 3)
        return unit, k

    def w_lhs(unit, k, slot):
        m = half_of(unit)

        def go(src, row):
            for j in range(2):
                copy(src.at[_ds(2 * row + j, T), _ds(m, T)], la.at[slot, :, pl.ds(j * T, T)], lsem.at[slot, j]).start()
        pl.when((unit > 0) & (unit < 5) & (k == 0))(lambda: go(x, 0))
        pl.when((unit > 0) & (unit < 5) & (k > 0))(lambda: go(xa, k - 1))
        pl.when(is_d(unit))(lambda: go(z, k))

    def w_lhs_wait(slot):
        for j in range(2):
            copy(x.at[pl.ds(0, T), pl.ds(0, T)], la.at[slot, :, pl.ds(j * T, T)], lsem.at[slot, j]).wait()

    def w_rhs(unit, k, slot):
        def go(src, row):
            copy(src.at[_ds(row, S), pl.ds(0, T)], wn.at[slot], rsem.at[slot, 0]).start()
            for j in range(2):
                copy(src.at[_ds(2 * row + j, T), pl.ds(T, T)], lb.at[slot, :, pl.ds(j * T, T)], rsem.at[slot, 1 + j]).start()
        pl.when(is_g(unit))(lambda: go(dug, k))
        pl.when(is_u(unit))(lambda: go(duu, k))
        pl.when(is_d(unit) & (k == 0))(lambda: go(dy, 0))
        pl.when(is_d(unit) & (k > 0))(lambda: go(dya, k - 1))

    def w_rhs_wait(slot):
        copy(x.at[:, pl.ds(0, T)], wn.at[slot], rsem.at[slot, 0]).wait()
        for j in range(2):
            copy(x.at[pl.ds(0, T), pl.ds(0, T)], lb.at[slot, :, pl.ds(j * T, T)], rsem.at[slot, 1 + j]).wait()

    def w_out(unit):
        def go(dst):
            for n in range(2):
                copy(acc.at[n], dst.at[_ds(half_of(unit), T), pl.ds(n * T, T)], asem.at[n]).start()
        pl.when(is_g(unit))(lambda: go(pg))
        pl.when(is_u(unit))(lambda: go(pu))
        pl.when(is_d(unit))(lambda: go(pd))

    def w_out_wait(n):
        copy(acc.at[n], pg.at[pl.ds(0, T), pl.ds(0, T)], asem.at[n]).wait()

    copy(dy.at[pl.ds(0, T)], lb.at[0], lsem.at[0, 1]).start()
    for c in f_rhs(0, 0):
        c.start()
    copy(x.at[pl.ds(0, T)], la.at[0], lsem.at[0, 0]).start()
    rcv[4] = jnp.zeros_like(rcv[4])
    bar = pltpu.get_barrier_semaphore()
    for dev in (sib, far):
        pl.semaphore_signal(bar, inc=1, device_id={"tp": dev}, device_id_type=MESH)
    pl.semaphore_wait(bar, 2)
    for q in range(4):
        for j in range(2):
            far_copy(q, j).start()

    def block(blk, carry):
        odd = jnp.where(blk == 3, 1, 0)
        dodd = jnp.where(blk == 2, 1, 0)
        n_w = jnp.where(blk == 1, 8, jnp.where(blk == 2, 5, jnp.where(blk == 3, 1, 0)))

        def f_step(i, carry):
            t, n, slot = 2 * blk + i // 4, i % 4, (i + odd) % 2
            ls = (i // 4 + odd) % 2

            @pl.when(blk == 3)
            def _():
                pl.when(i == 1)(lambda: forward(3, 0))
                pl.when(i == 2)(lambda: forward(3, 1))
            pl.when(n == 0)(lambda: f_lhs_wait(ls))
            for c in f_rhs(n, slot):
                c.wait()

            @pl.when((i < 7) | (blk == 0))
            def _():
                for c in f_rhs((n + 1) % 4, 1 - slot):
                    c.start()

            @pl.when((i < 4) | (blk == 0))
            def _():
                pl.when(n == 2)(lambda: f_lhs(t + 1, 1 - ls, 0))
                pl.when(n == 3)(lambda: f_lhs(t + 1, 1 - ls, 1))

            @pl.when((i == 7) & (blk > 0))
            def _():
                unit, k = w_of(blk, 0)
                w_lhs(unit, k, odd)
                w_rhs(unit, k, odd)

            @pl.when(blk == 0)
            def _():
                for j in range(2):
                    sib_copy(i, j).start()

            @pl.when((i >= 2) | (blk == 1))
            def _():
                for c in f_outs(t, n, slot):
                    c.wait()

            @pl.when((i < 2) & (blk == 2))
            def _():
                for h in range(2):
                    d_send_own(1, i, slot, h).wait_send()

            @pl.when((i < 2) & (blk == 3))
            def _():
                for h in range(2):
                    d_out(s01, i, slot, h).wait()
                pl.when(i == 1)(lambda: s_copy().start())

            _gate(la.at[ls], lb.at[ls], wn.at[slot], wt.at[slot, 0], ob.at[slot])
            for c in f_outs(t, n, slot):
                c.start()
            return carry

        lax.fori_loop(0, 8, f_step, 0)

        def w_step(grp, carry):
            unit, k = w_of(blk, grp)
            ls = (grp + odd) % 2
            last = jnp.where(unit < 4, 1, 2)

            w_lhs_wait(ls)
            w_rhs_wait(ls)

            @pl.when((grp == 1) & (blk < 3) | (blk == 3))
            def _():
                for s in range(2):
                    for c in f_outs(0, 0, s):
                        c.wait()

            @pl.when(grp + 1 < n_w)
            def _():
                unit2, k2 = w_of(blk, grp + 1)
                w_lhs(unit2, k2, 1 - ls)
                w_rhs(unit2, k2, 1 - ls)

            @pl.when(grp + 1 == n_w)
            def _():
                d_lhs(blk, 0, 1 - ls)
                for c in d_rhs(0, 1 - ls):
                    c.start()

            for j in range(2):
                pl.when((blk == 1) & (grp == j))(lambda: forward(0, j))
                pl.when((blk == 2) & (grp == 1 + j))(lambda: forward(2, j))

            @pl.when((k == 0) & (unit > 0))
            def _():
                for n in range(2):
                    w_out_wait(n)
            _wgrad(acc, 0, la.at[ls], wn.at[ls], lb.at[ls], k > 0)
            pl.when(k == last)(lambda: w_out(unit))
            return carry

        lax.fori_loop(0, n_w, w_step, 0)

        def d_step(i, carry):
            g, n, slot = i // 2, i % 2, (i + dodd) % 2
            ls = (g + dodd) % 2
            mine = (blk > 1) & (g == 1)

            pl.when(n == 0)(lambda: d_lhs_wait(ls))
            for c in d_rhs(n, slot):
                c.wait()

            @pl.when(mine)
            def _():
                for h in range(2):
                    d_send_far(blk, n, slot, h).wait_recv()

            @pl.when(i < 3)
            def _():
                for c in d_rhs(1 - n, 1 - slot):
                    c.start()
            pl.when(i == 0)(lambda: d_lhs(blk, 1, 1 - ls))

            @pl.when(blk < 3)
            def _():
                pl.when(i == 2)(lambda: f_lhs(2 * blk + 2, 1 - ls, 0))

                @pl.when(i == 3)
                def _():
                    for c in f_rhs(0, 1 - slot):
                        c.start()
                    f_lhs(2 * blk + 2, 1 - ls, 1)

            for j in range(2):
                pl.when((blk == 1) & (i == 1 + j))(lambda: forward(1, j))

            @pl.when(i >= 2)
            def _():
                for h in range(2):
                    d_send_own(0, n, slot, h).wait_send()

            p = [_dot(la[ls, :, pl.ds(0, T)], wn[slot, pl.ds(h * C, C)], NT)
                 + _dot(la[ls, :, pl.ds(T, T)], wn[slot, pl.ds(T + h * C, C)], NT) + _dot(lb[ls], wt[slot, h], NT) for h in range(2)]
            for h in range(2):
                ob[slot, h] = (p[h] + rcv[jnp.where(mine, 2 * n + h, 4)].astype(F32)).astype(BF16)
            for h in range(2):
                pl.when(blk == 1)(lambda: d_send_own(g, n, slot, h).start())
                pl.when((blk > 1) & (g == 0))(lambda: d_send_far(blk, n, slot, h).start())
                pl.when(mine & (blk == 2))(lambda: d_out(s01, n, slot, h).start())
                pl.when(mine & (blk == 3))(lambda: d_out(s23, n, slot, h).start())
            return carry

        @pl.when(blk > 0)
        def _():
            lax.fori_loop(0, 4, d_step, 0)
        return carry

    lax.fori_loop(0, 4, block, 0)

    for s in range(2):
        for h in range(2):
            d_out(s23, s, s, h).wait()
        w_out_wait(s)
    for i in range(8):
        for j in range(2):
            sib_copy(i, j).wait_send()
    for q in range(4):
        for j in range(2):
            far_copy(q, j).wait_send()
            fwd_copy(q, j).wait_send()
    for i in range(8):
        d_send_own(i // 4, i // 2 % 2, 0, i % 2).wait_recv()
    s_copy().wait()


def _k2(dya, xa, z, dug, duu, psib, r01, wg, wu, pg, pu, pd, dwg, dwu, dwd, dx,
        la, lb, wn, ob, acc, add, lsem, rsem, osem, asem, psem, dsem):
    copy = pltpu.make_async_copy
    n_w = 10

    def w_of(grp):
        pos = sum(jnp.where(grp >= g, 1, 0) for g in (2, 3, 5, 7, 8))
        k = 3 - sum(jnp.where(grp == g, 1, 0) for g in (0, 3, 5, 8))
        return unit_of(pos), pos, k

    def unit_of(pos):
        return jnp.where(pos == 1, 4, jnp.where(pos == 4, 5, pos - jnp.where(pos > 4, 2, jnp.where(pos > 1, 1, 0))))

    def w_lhs(unit, k, slot):
        def go(src, row):
            for j in range(2):
                copy(src.at[_ds(2 * row + j, T), _ds(half_of(unit), T)], la.at[slot, :, pl.ds(j * T, T)], lsem.at[slot, j]).start()
        pl.when((unit > 0) & (unit < 5))(lambda: go(xa, k - 1))
        pl.when(is_d(unit))(lambda: go(z, k))

    def w_rhs(unit, k, slot):
        def go(src, row):
            copy(src.at[_ds(row, S), pl.ds(0, T)], wn.at[slot], rsem.at[slot, 0]).start()
            for j in range(2):
                copy(src.at[_ds(2 * row + j, T), pl.ds(T, T)], lb.at[slot, :, pl.ds(j * T, T)], rsem.at[slot, 1 + j]).start()
        pl.when(is_g(unit))(lambda: go(dug, k))
        pl.when(is_u(unit))(lambda: go(duu, k))
        pl.when(is_d(unit))(lambda: go(dya, k - 1))

    def w_wait(slot):
        copy(dug.at[pl.ds(0, S), pl.ds(0, T)], wn.at[slot], rsem.at[slot, 0]).wait()
        for j in range(2):
            copy(xa.at[pl.ds(0, T), pl.ds(0, T)], la.at[slot, :, pl.ds(j * T, T)], lsem.at[slot, j]).wait()
            copy(xa.at[pl.ds(0, T), pl.ds(0, T)], lb.at[slot, :, pl.ds(j * T, T)], rsem.at[slot, 1 + j]).wait()

    def w_tile(unit, n):
        return _ds(half_of(unit), T), pl.ds(n * T, T)

    def w_part(pos):
        unit = unit_of(pos)

        def go(src):
            for n in range(2):
                a = 2 * (pos % 3) + n
                copy(src.at[w_tile(unit, n)], acc.at[a], psem.at[a]).start()
        pl.when(is_g(unit))(lambda: go(pg))
        pl.when(is_u(unit))(lambda: go(pu))
        pl.when(is_d(unit))(lambda: go(pd))

    def w_part_wait(pos):
        for n in range(2):
            a = 2 * (pos % 3) + n
            copy(pg.at[w_tile(0, n)], acc.at[a], psem.at[a]).wait()

    def w_out(pos):
        unit = unit_of(pos)

        def go(dst):
            for n in range(2):
                a = 2 * (pos % 3) + n
                copy(acc.at[a], dst.at[w_tile(unit, n)], asem.at[a]).start()
        pl.when(is_g(unit))(lambda: go(dwg))
        pl.when(is_u(unit))(lambda: go(dwu))
        pl.when(is_d(unit))(lambda: go(dwd))

    def w_out_wait(pos):
        for n in range(2):
            a = 2 * (pos % 3) + n
            copy(acc.at[a], dwg.at[w_tile(0, n)], asem.at[a]).wait()

    def d_lhs(slot):
        return (copy(dug.at[pl.ds(0, T)], la.at[slot], lsem.at[slot, 0]),
                copy(duu.at[pl.ds(0, T)], lb.at[slot], lsem.at[slot, 1]))

    def d_rhs(n, slot):
        return [copy(w.at[_ds(n, C), pl.ds(j * T, T)], wn.at[slot, pl.ds((2 * k + j) * C, C)], rsem.at[slot, 2 * k + j])
                for k, w in enumerate((wg, wu)) for j in range(2)] + [
            copy(psib.at[pl.ds(0, T), _ds(n, C)], add.at[slot, 0], dsem.at[slot, 0]),
            copy(r01.at[:, _ds(n, C)], add.at[slot, 1], dsem.at[slot, 1])]

    def d_out(n, slot):
        return copy(ob.at[slot], dx.at[pl.ds(0, T), _ds(n, C)], osem.at[slot])

    w_lhs(0, 2, 0)
    w_rhs(0, 2, 0)
    w_part(0)

    def w_step(grp, carry):
        unit, pos, k = w_of(grp)
        ls = grp % 2
        w_wait(ls)

        @pl.when(grp + 1 < n_w)
        def _():
            unit2, _, k2 = w_of(grp + 1)
            w_lhs(unit2, k2, 1 - ls)
            w_rhs(unit2, k2, 1 - ls)

        @pl.when(grp + 1 == n_w)
        def _():
            for c in (*d_lhs(0), *d_rhs(0, 0)):
                c.start()

        pl.when((k == 2) | (unit >= 4))(lambda: w_part_wait(pos))

        @pl.when((k == 3) & (pos < 5))
        def _():
            pl.when(pos > 1)(lambda: w_out_wait(pos + 1))
            w_part(pos + 1)
        _wgrad(acc, 2 * (pos % 3), la.at[ls], wn.at[ls], lb.at[ls], None)
        pl.when(k == 3)(lambda: w_out(pos))
        return carry

    lax.fori_loop(0, n_w, w_step, 0)

    def d_step(n, carry):
        slot = n % 2

        @pl.when(n == 0)
        def _():
            for c in d_lhs(0):
                c.wait()
        for c in d_rhs(n, slot):
            c.wait()

        @pl.when(n < 3)
        def _():
            for c in d_rhs(n + 1, 1 - slot):
                c.start()
        pl.when(n >= 2)(lambda: d_out(n, slot).wait())
        p = sum(_dot(lhs[0, :, pl.ds(j * T, T)], wn[slot, pl.ds((2 * k + j) * C, C)], NT)
                for k, lhs in enumerate((la, lb)) for j in range(2))
        ob[slot] = (p + add[slot, 0].astype(F32) + add[slot, 1].astype(F32)).astype(BF16)
        d_out(n, slot).start()
        return carry

    lax.fori_loop(0, 4, d_step, 0)
    for s in range(2):
        d_out(2 + s, s).wait()
    for pos in range(3):
        w_out_wait(pos)


def _k3(dug, duu, wg, wu, psib, r23, _, dx, la, lb, wt, add, ob, lsem, rsem, dsem, osem):
    copy = pltpu.make_async_copy

    def lhs(m):
        return (copy(dug.at[_ds(2 + m, C)], la.at[m], lsem.at[m, 0]), copy(duu.at[_ds(2 + m, C)], lb.at[m], lsem.at[m, 1]))

    def rhs(n, slot):
        return (copy(wg.at[_ds(n, C)], wt.at[slot, 0], rsem.at[slot, 0]), copy(wu.at[_ds(n, C)], wt.at[slot, 1], rsem.at[slot, 1]))

    def adds(m, n, slot):
        return (copy(psib.at[_ds(2 + m, C), _ds(n, C)], add.at[slot, 0], dsem.at[slot, 0]),
                copy(r23.at[_ds(m, C), _ds(n, C)], add.at[slot, 1], dsem.at[slot, 1]))

    def out(m, n, slot):
        return copy(ob.at[slot], dx.at[_ds(2 + m, C), _ds(n, C)], osem.at[slot])

    for c in (*lhs(0), *rhs(0, 0), *adds(0, 0, 0), *lhs(1)):
        c.start()

    def step(i, carry):
        n, m, slot = i // 2, i % 2, i // 2 % 2

        @pl.when(i < 2)
        def _():
            for c in lhs(m):
                c.wait()

        @pl.when(m == 0)
        def _():
            for c in rhs(n, slot):
                c.wait()

            @pl.when(n < 3)
            def _():
                for c in rhs(n + 1, 1 - slot):
                    c.start()
        for c in adds(m, n, m):
            c.wait()

        @pl.when(i < 7)
        def _():
            for c in adds(1 - m, n + m, 1 - m):
                c.start()
        pl.when(i >= 2)(lambda: out(m, n, m).wait())
        p = _dot(la[m], wt[slot, 0], NT) + _dot(lb[m], wt[slot, 1], NT)
        ob[m] = (p + add[m, 0].astype(F32) + add[m, 1].astype(F32)).astype(BF16)
        out(m, n, m).start()
        return carry

    lax.fori_loop(0, 8, step, 0)
    for m in range(2):
        out(m, 3, m).wait()


def _local(x, dy, wg, wu, wd):
    def bf(r):
        return jax.ShapeDtypeStruct((r, S), BF16)

    def ff(r):
        return jax.ShapeDtypeStruct((r, S), F32)
    k1 = pl.pallas_call(
        _k1, name="gather_gate",
        out_shape=(bf(3 * S), bf(3 * S), bf(4 * S), bf(4 * S), bf(4 * S), bf(S), bf(T), bf(T), bf(T), ff(S), ff(S), ff(S)),
        in_specs=[ANY] * 5, out_specs=(ANY,) * 12,
        scratch_shapes=[pltpu.VMEM((2, T, S), BF16), pltpu.VMEM((2, T, S), BF16), pltpu.VMEM((2, S, T), BF16),
                        pltpu.VMEM((2, 2, C, S), BF16), pltpu.VMEM((2, 3, T, C), BF16), pltpu.VMEM((2, T, T), F32),
                        pltpu.VMEM((5, T, C), BF16), DMA((2, 4)), DMA((2, 4)), DMA((2, 3)), DMA((2,)),
                        DMA((8,)), DMA((8,)), DMA((16,)), DMA((16,)), DMA((8,)), DMA((8,)), DMA((2, 2)), DMA((16,)),
                        DMA((1,)), DMA((1,))],
        cost_estimate=pl.CostEstimate(flops=420_000_000_000, bytes_accessed=1 << 30, transcendentals=0),
        compiler_params=pltpu.CompilerParams(collective_id=0, has_side_effects=True, vmem_limit_bytes=VMEM))
    xa, dya, z, dug, duu, psib, _, s23, r01, pg, pu, pd = k1(x, dy, wg, wu, wd)
    r23 = lax.ppermute(s23, "tp", [(0, 2), (2, 0), (1, 3), (3, 1)])
    k2 = pl.pallas_call(
        _k2, name="wgrad_dx",
        out_shape=(ff(S), ff(S), ff(S), bf(S)),
        in_specs=[ANY] * 12, out_specs=(ANY,) * 4,
        scratch_shapes=[pltpu.VMEM((2, T, S), BF16), pltpu.VMEM((2, T, S), BF16), pltpu.VMEM((2, S, T), BF16),
                        pltpu.VMEM((2, T, C), BF16), pltpu.VMEM((6, T, T), F32),
                        pltpu.VMEM((2, 2, T, C), BF16), DMA((2, 2)), DMA((2, 4)), DMA((2,)), DMA((6,)), DMA((6,)), DMA((2, 2))],
        cost_estimate=pl.CostEstimate(flops=105_000_000_000, bytes_accessed=1 << 28, transcendentals=0),
        compiler_params=pltpu.CompilerParams(vmem_limit_bytes=VMEM))
    dwg, dwu, dwd, dx = k2(dya, xa, z, dug, duu, psib, r01, wg, wu, pg, pu, pd)
    dx = pl.pallas_call(
        _k3, name="dx", out_shape=bf(S), in_specs=[ANY] * 7, out_specs=ANY, input_output_aliases={6: 0},
        scratch_shapes=[pltpu.VMEM((2, C, S), BF16), pltpu.VMEM((2, C, S), BF16), pltpu.VMEM((2, 2, C, S), BF16),
                        pltpu.VMEM((2, 2, C, C), BF16), pltpu.VMEM((2, C, C), BF16), DMA((2, 2)), DMA((2, 2)), DMA((2, 2)), DMA((2,))],
        cost_estimate=pl.CostEstimate(flops=4 * T * S * S, bytes_accessed=1 << 25, transcendentals=0),
        compiler_params=pltpu.CompilerParams(vmem_limit_bytes=VMEM))(dug, duu, wg, wu, psib, r23, dx)
    return dx, dwg, dwu, dwd


def solution(mesh):
    rows = P(("dp", "tp"), None)
    return jax.shard_map(_local, mesh=mesh,
                         in_specs=(rows, rows, P(None, "tp"), P(None, "tp"), P("tp", None)),
                         out_specs=(rows, P("dp", "tp"), P("dp", "tp"), rows),
                         check_vma=False)
```

```python
import jax
import jax.numpy as jnp
from jax import lax
from jax.experimental import pallas as pl
from jax.experimental.pallas import tpu as pltpu
from jax.sharding import PartitionSpec as P

F32, BF16 = jnp.float32, jnp.bfloat16
NN = (((1,), (0,)), ((), ()))
NT = (((1,), (1,)), ((), ()))
TN = (((0,), (0,)), ((), ()))
ANY = pl.BlockSpec(memory_space=pl.ANY)
MESH = pl.DeviceIdType.MESH
DMA = pltpu.SemaphoreType.DMA

S = 2048
T = 1024
C = 512
P8 = 256
VMEM = 67043328


def _dot(a, b, dims):
    return lax.dot_general(a, b, dims, preferred_element_type=F32)


def _ds(i, n):
    return pl.ds(pl.multiple_of(i * n, n), n)


def _gate(la, lb, wn, wt, ob):
    g = _dot(lb[...], wt[...], NT)
    ug = _dot(la[...], wn[:, pl.ds(0, C)], NN).astype(BF16).astype(F32)
    s = jax.nn.sigmoid(ug)
    a = ug * s
    ob[2] = (g * a).astype(BF16)
    gd = g * (s * (1.0 + ug * (1.0 - s)))
    uu = _dot(la[...], wn[:, pl.ds(C, C)], NN).astype(BF16).astype(F32)
    ob[0] = (a * uu).astype(BF16)
    ob[1] = (gd * uu).astype(BF16)


def _wgrad(old, n, la, wn, lb):
    rhs = (wn[pl.ds(0, T), :], wn[pl.ds(T, T), :]) if n == 0 else (lb[:, pl.ds(0, T)], lb[:, pl.ds(T, T)])
    return old + _dot(la[:, pl.ds(0, T)], rhs[0], TN) + _dot(la[:, pl.ds(T, T)], rhs[1], TN)


def half_of(unit):
    return jnp.where((unit == 2) | (unit >= 4), 1, 0)


def is_d(unit):
    return (unit == 0) | (unit == 5)


def is_g(unit):
    return (unit == 1) | (unit == 2)


def is_u(unit):
    return (unit == 3) | (unit == 4)


def _k1(x, dy, wg, wu, wd, xa, dya, z, dug, duu, psib, s01, s23, r01, pg, pu, pd,
        la, lb, wn, wt, ob, acc, rcv, lsem, rsem, osem, asem,
        far_s, far_r, sib_s, sib_r, fwd_s, fwd_r, p_s, p_r, s_s, s_r):
    me = lax.axis_index("tp")
    sib = me // 2 * 2 + 1 - me % 2
    far = (me + 2) % 4
    copy = pltpu.make_async_copy

    def remote(src, dst, ss, rs, dev):
        return pltpu.make_async_remote_copy(src_ref=src, dst_ref=dst, send_sem=ss, recv_sem=rs,
                                            device_id={"tp": dev}, device_id_type=MESH)

    def far_copy(q, j):
        src, dst = ((x, xa), (dy, dya))[j]
        return remote(src.at[pl.ds(q * C, C)], dst.at[pl.ds(S + q * T, C)], far_s.at[2 * q + j], far_r.at[2 * q + j], far)

    def sib_copy(i, j):
        src, dst = ((x, xa), (dy, dya))[j]
        return remote(src.at[_ds(i, P8)], dst.at[_ds(i, P8)], sib_s.at[2 * i + j], sib_r.at[2 * i + j], sib)

    def fwd_copy(q, j):
        buf = (xa, dya)[j]
        return remote(buf.at[_ds(4 + 2 * q, C)], buf.at[_ds(5 + 2 * q, C)], fwd_s.at[2 * q + j], fwd_r.at[2 * q + j], sib)

    def forward(q, j):
        far_copy(q, j).wait_recv()
        fwd_copy(q, j).start()

    def s_copy():
        return remote(s01, r01, s_s.at[0], s_r.at[0], far)

    def f_lhs(t, slot, j):
        own, all_, buf = ((x, xa, la), (dy, dya, lb))[j]

        @pl.when((t == 2) | (t == 3))
        def _():
            for i in range(4):
                sib_copy(4 * (t - 2) + i, j).wait_recv()
        pl.when(t >= 4)(lambda: fwd_copy(t - 4, j).wait_recv())
        pl.when(t < 2)(lambda: copy(own.at[_ds(t, T)], buf.at[slot], lsem.at[slot, j]).start())
        pl.when(t >= 2)(lambda: copy(all_.at[_ds(t - 2, T)], buf.at[slot], lsem.at[slot, j]).start())

    def f_lhs_wait(slot):
        copy(x.at[pl.ds(0, T)], la.at[slot], lsem.at[slot, 0]).wait()
        copy(dy.at[pl.ds(0, T)], lb.at[slot], lsem.at[slot, 1]).wait()

    def f_rhs(n, slot):
        return (copy(wg.at[:, _ds(n, C)], wn.at[slot, :, pl.ds(0, C)], rsem.at[slot, 0]),
                copy(wu.at[:, _ds(n, C)], wn.at[slot, :, pl.ds(C, C)], rsem.at[slot, 1]),
                copy(wd.at[_ds(n, C)], wt.at[slot, 0], rsem.at[slot, 2]))

    def f_outs(t, n, slot):
        return [copy(ob.at[slot, j], dst.at[_ds(t, T), _ds(n, C)], osem.at[slot, j]) for j, dst in enumerate((z, dug, duu))]

    def d_lhs(blk, g, slot):
        for j in range(2):
            row = jnp.where(blk == 1, 4 + 2 * g + j, 8 + 2 * (2 * (blk - 2) + j) + 1 - g)
            copy(dug.at[_ds(row, C)], la.at[slot, pl.ds(j * C, C)], lsem.at[slot, 2 * j]).start()
            copy(duu.at[_ds(row, C)], lb.at[slot, pl.ds(j * C, C)], lsem.at[slot, 2 * j + 1]).start()

    def d_lhs_wait(slot):
        for j in range(2):
            copy(dug.at[pl.ds(0, C)], la.at[slot, pl.ds(j * C, C)], lsem.at[slot, 2 * j]).wait()
            copy(duu.at[pl.ds(0, C)], lb.at[slot, pl.ds(j * C, C)], lsem.at[slot, 2 * j + 1]).wait()

    def d_rhs(n, slot):
        return [copy(wg.at[_ds(n, T), pl.ds(j * T, T)], wn.at[slot, pl.ds(j * T, T)], rsem.at[slot, j]) for j in range(2)] + [
            copy(wu.at[_ds(2 * n + j, C)], wt.at[slot, j], rsem.at[slot, 2 + j]) for j in range(2)]

    def d_send_own(g, n, slot, h):
        return remote(ob.at[slot, h], psib.at[_ds(g, T), _ds(2 * n + h, C)], p_s.at[slot, h], p_r.at[4 * g + 2 * n + h], sib)

    def d_send_far(blk, n, slot, h):
        return remote(ob.at[slot, h], rcv.at[2 * n + h], p_s.at[slot, h], p_r.at[4 * blk + 2 * n + h], sib)

    def d_out(dst, n, slot, h):
        return copy(ob.at[slot, h], dst.at[:, _ds(2 * n + h, C)], osem.at[slot, h])

    def w_of(blk, grp):
        h = jnp.where(blk == 3, 5, grp)
        unit = jnp.where(blk == 1, grp // 2, 4 + h // 3)
        k = jnp.where(blk == 1, grp % 2, h % 3)
        return unit, k

    def w_lhs(unit, k, slot):
        m = half_of(unit)

        def go(src, row):
            for j in range(2):
                copy(src.at[_ds(2 * row + j, T), _ds(m, T)], la.at[slot, :, pl.ds(j * T, T)], lsem.at[slot, j]).start()
        pl.when((unit > 0) & (unit < 5) & (k == 0))(lambda: go(x, 0))
        pl.when((unit > 0) & (unit < 5) & (k > 0))(lambda: go(xa, k - 1))
        pl.when(is_d(unit))(lambda: go(z, k))

    def w_lhs_wait(slot):
        for j in range(2):
            copy(x.at[pl.ds(0, T), pl.ds(0, T)], la.at[slot, :, pl.ds(j * T, T)], lsem.at[slot, j]).wait()

    def w_rhs(unit, k, slot):
        def go(src, row):
            copy(src.at[_ds(row, S), pl.ds(0, T)], wn.at[slot], rsem.at[slot, 0]).start()
            for j in range(2):
                copy(src.at[_ds(2 * row + j, T), pl.ds(T, T)], lb.at[slot, :, pl.ds(j * T, T)], rsem.at[slot, 1 + j]).start()
        pl.when(is_g(unit))(lambda: go(dug, k))
        pl.when(is_u(unit))(lambda: go(duu, k))
        pl.when(is_d(unit) & (k == 0))(lambda: go(dy, 0))
        pl.when(is_d(unit) & (k > 0))(lambda: go(dya, k - 1))

    def w_rhs_wait(slot):
        copy(x.at[:, pl.ds(0, T)], wn.at[slot], rsem.at[slot, 0]).wait()
        for j in range(2):
            copy(x.at[pl.ds(0, T), pl.ds(0, T)], lb.at[slot, :, pl.ds(j * T, T)], rsem.at[slot, 1 + j]).wait()

    def w_out(unit, n):
        def go(dst):
            copy(acc.at[n], dst.at[_ds(half_of(unit), T), pl.ds(n * T, T)], asem.at[n]).start()
        pl.when(is_g(unit))(lambda: go(pg))
        pl.when(is_u(unit))(lambda: go(pu))
        pl.when(is_d(unit))(lambda: go(pd))

    def w_out_wait(n):
        copy(acc.at[n], pg.at[pl.ds(0, T), pl.ds(0, T)], asem.at[n]).wait()

    copy(dy.at[pl.ds(0, T)], lb.at[0], lsem.at[0, 1]).start()
    for c in f_rhs(0, 0):
        c.start()
    copy(x.at[pl.ds(0, T)], la.at[0], lsem.at[0, 0]).start()
    rcv[4] = jnp.zeros_like(rcv[4])
    bar = pltpu.get_barrier_semaphore()
    for dev in (sib, far):
        pl.semaphore_signal(bar, inc=1, device_id={"tp": dev}, device_id_type=MESH)
    pl.semaphore_wait(bar, 2)
    for q in range(4):
        for j in range(2):
            far_copy(q, j).start()

    def block(blk, carry):
        odd = jnp.where(blk == 3, 1, 0)
        dodd = jnp.where(blk == 2, 1, 0)
        n_w = jnp.where(blk == 1, 8, jnp.where(blk == 2, 5, jnp.where(blk == 3, 1, 0)))

        def f_step(i, carry):
            t, n, slot = 2 * blk + i // 4, i % 4, (i + odd) % 2
            ls = (i // 4 + odd) % 2

            @pl.when(blk == 3)
            def _():
                pl.when(i == 1)(lambda: forward(3, 0))
                pl.when(i == 2)(lambda: forward(3, 1))
            pl.when(n == 0)(lambda: f_lhs_wait(ls))
            for c in f_rhs(n, slot):
                c.wait()

            @pl.when((i < 7) | (blk == 0))
            def _():
                for c in f_rhs((n + 1) % 4, 1 - slot):
                    c.start()

            @pl.when((i < 4) | (blk == 0))
            def _():
                pl.when(n == 2)(lambda: f_lhs(t + 1, 1 - ls, 0))
                pl.when(n == 3)(lambda: f_lhs(t + 1, 1 - ls, 1))

            @pl.when((i == 7) & (blk > 0))
            def _():
                unit, k = w_of(blk, 0)
                w_lhs(unit, k, odd)
                w_rhs(unit, k, odd)

            @pl.when(blk == 0)
            def _():
                for j in range(2):
                    sib_copy(i, j).start()

            @pl.when((i >= 2) | (blk == 1))
            def _():
                for c in f_outs(t, n, slot):
                    c.wait()

            @pl.when((i < 2) & (blk == 2))
            def _():
                for h in range(2):
                    d_send_own(1, i, slot, h).wait_send()

            @pl.when((i < 2) & (blk == 3))
            def _():
                for h in range(2):
                    d_out(s01, i, slot, h).wait()
                pl.when(i == 1)(lambda: s_copy().start())

            _gate(la.at[ls], lb.at[ls], wn.at[slot], wt.at[slot, 0], ob.at[slot])
            for c in f_outs(t, n, slot):
                c.start()
            return carry

        lax.fori_loop(0, 8, f_step, 0)

        def w_step(grp, carry):
            unit, k = w_of(blk, grp)
            ls = (grp + odd) % 2
            last = jnp.where(unit < 4, 1, 2)

            w_lhs_wait(ls)
            w_rhs_wait(ls)

            @pl.when((grp == 1) & (blk < 3) | (blk == 3))
            def _():
                for s in range(2):
                    for c in f_outs(0, 0, s):
                        c.wait()

            @pl.when(grp + 1 < n_w)
            def _():
                unit2, k2 = w_of(blk, grp + 1)
                w_lhs(unit2, k2, 1 - ls)
                w_rhs(unit2, k2, 1 - ls)

            @pl.when(grp + 1 == n_w)
            def _():
                d_lhs(blk, 0, 1 - ls)
                for c in d_rhs(0, 1 - ls):
                    c.start()

            for j in range(2):
                pl.when((blk == 1) & (grp == j))(lambda: forward(0, j))
                pl.when((blk == 2) & (grp == 1 + j))(lambda: forward(2, j))

            for n in range(2):
                pl.when((k == 0) & (unit > 0))(lambda: w_out_wait(n))
                acc[n] = _wgrad(jnp.where(k > 0, acc[n], 0.0), n, la.at[ls], wn.at[ls], lb.at[ls])
                pl.when(k == last)(lambda: w_out(unit, n))
            return carry

        lax.fori_loop(0, n_w, w_step, 0)

        def d_step(i, carry):
            g, n, slot = i // 2, i % 2, (i + dodd) % 2
            ls = (g + dodd) % 2
            mine = (blk > 1) & (g == 1)

            pl.when(n == 0)(lambda: d_lhs_wait(ls))
            for c in d_rhs(n, slot):
                c.wait()

            @pl.when(mine)
            def _():
                for h in range(2):
                    d_send_far(blk, n, slot, h).wait_recv()

            @pl.when(i < 3)
            def _():
                for c in d_rhs(1 - n, 1 - slot):
                    c.start()
            pl.when(i == 0)(lambda: d_lhs(blk, 1, 1 - ls))

            @pl.when(blk < 3)
            def _():
                pl.when(i == 2)(lambda: f_lhs(2 * blk + 2, 1 - ls, 0))

                @pl.when(i == 3)
                def _():
                    for c in f_rhs(0, 1 - slot):
                        c.start()
                    f_lhs(2 * blk + 2, 1 - ls, 1)

            for j in range(2):
                pl.when((blk == 1) & (i == 1 + j))(lambda: forward(1, j))

            @pl.when(i >= 2)
            def _():
                for h in range(2):
                    d_send_own(0, n, slot, h).wait_send()

            p = [_dot(la[ls, :, pl.ds(0, T)], wn[slot, pl.ds(h * C, C)], NT)
                 + _dot(la[ls, :, pl.ds(T, T)], wn[slot, pl.ds(T + h * C, C)], NT) + _dot(lb[ls], wt[slot, h], NT) for h in range(2)]
            for h in range(2):
                ob[slot, h] = (p[h] + rcv[jnp.where(mine, 2 * n + h, 4)].astype(F32)).astype(BF16)
            for h in range(2):
                pl.when(blk == 1)(lambda: d_send_own(g, n, slot, h).start())
                pl.when((blk > 1) & (g == 0))(lambda: d_send_far(blk, n, slot, h).start())
                pl.when(mine & (blk == 2))(lambda: d_out(s01, n, slot, h).start())
                pl.when(mine & (blk == 3))(lambda: d_out(s23, n, slot, h).start())
            return carry

        @pl.when(blk > 0)
        def _():
            lax.fori_loop(0, 4, d_step, 0)
        return carry

    lax.fori_loop(0, 4, block, 0)

    for s in range(2):
        for h in range(2):
            d_out(s23, s, s, h).wait()
        w_out_wait(s)
    for i in range(8):
        for j in range(2):
            sib_copy(i, j).wait_send()
    for q in range(4):
        for j in range(2):
            far_copy(q, j).wait_send()
            fwd_copy(q, j).wait_send()
    for i in range(8):
        d_send_own(i // 4, i // 2 % 2, 0, i % 2).wait_recv()
    s_copy().wait()


def _k2(dya, xa, z, dug, duu, psib, r01, wg, wu, pg, pu, pd, dwg, dwu, dwd, dx,
        la, lb, wn, ob, acc, add, lsem, rsem, osem, asem, psem, dsem):
    copy = pltpu.make_async_copy
    n_w = 10

    def w_of(grp):
        pos = sum(jnp.where(grp >= g, 1, 0) for g in (2, 3, 5, 7, 8))
        k = 3 - sum(jnp.where(grp == g, 1, 0) for g in (0, 3, 5, 8))
        return unit_of(pos), pos, k

    def unit_of(pos):
        return jnp.where(pos == 1, 4, jnp.where(pos == 4, 5, pos - jnp.where(pos > 4, 2, jnp.where(pos > 1, 1, 0))))

    def w_lhs(unit, k, slot):
        def go(src, row):
            for j in range(2):
                copy(src.at[_ds(2 * row + j, T), _ds(half_of(unit), T)], la.at[slot, :, pl.ds(j * T, T)], lsem.at[slot, j]).start()
        pl.when((unit > 0) & (unit < 5))(lambda: go(xa, k - 1))
        pl.when(is_d(unit))(lambda: go(z, k))

    def w_rhs(unit, k, slot):
        def go(src, row):
            copy(src.at[_ds(row, S), pl.ds(0, T)], wn.at[slot], rsem.at[slot, 0]).start()
            for j in range(2):
                copy(src.at[_ds(2 * row + j, T), pl.ds(T, T)], lb.at[slot, :, pl.ds(j * T, T)], rsem.at[slot, 1 + j]).start()
        pl.when(is_g(unit))(lambda: go(dug, k))
        pl.when(is_u(unit))(lambda: go(duu, k))
        pl.when(is_d(unit))(lambda: go(dya, k - 1))

    def w_wait(slot):
        copy(dug.at[pl.ds(0, S), pl.ds(0, T)], wn.at[slot], rsem.at[slot, 0]).wait()
        for j in range(2):
            copy(xa.at[pl.ds(0, T), pl.ds(0, T)], la.at[slot, :, pl.ds(j * T, T)], lsem.at[slot, j]).wait()
            copy(xa.at[pl.ds(0, T), pl.ds(0, T)], lb.at[slot, :, pl.ds(j * T, T)], rsem.at[slot, 1 + j]).wait()

    def w_tile(unit, n):
        return _ds(half_of(unit), T), pl.ds(n * T, T)

    def w_part(pos):
        unit = unit_of(pos)

        def go(src):
            for n in range(2):
                a = 2 * (pos % 3) + n
                copy(src.at[w_tile(unit, n)], acc.at[a], psem.at[a]).start()
        pl.when(is_g(unit))(lambda: go(pg))
        pl.when(is_u(unit))(lambda: go(pu))
        pl.when(is_d(unit))(lambda: go(pd))

    def w_part_wait(pos):
        for n in range(2):
            a = 2 * (pos % 3) + n
            copy(pg.at[w_tile(0, n)], acc.at[a], psem.at[a]).wait()

    def w_out(pos):
        unit = unit_of(pos)

        def go(dst):
            for n in range(2):
                a = 2 * (pos % 3) + n
                copy(acc.at[a], dst.at[w_tile(unit, n)], asem.at[a]).start()
        pl.when(is_g(unit))(lambda: go(dwg))
        pl.when(is_u(unit))(lambda: go(dwu))
        pl.when(is_d(unit))(lambda: go(dwd))

    def w_out_wait(pos):
        for n in range(2):
            a = 2 * (pos % 3) + n
            copy(acc.at[a], dwg.at[w_tile(0, n)], asem.at[a]).wait()

    def d_lhs(slot):
        return (copy(dug.at[pl.ds(0, T)], la.at[slot], lsem.at[slot, 0]),
                copy(duu.at[pl.ds(0, T)], lb.at[slot], lsem.at[slot, 1]))

    def d_rhs(n, slot):
        return [copy(w.at[_ds(n, C), pl.ds(j * T, T)], wn.at[slot, pl.ds((2 * k + j) * C, C)], rsem.at[slot, 2 * k + j])
                for k, w in enumerate((wg, wu)) for j in range(2)] + [
            copy(psib.at[pl.ds(0, T), _ds(n, C)], add.at[slot, 0], dsem.at[slot, 0]),
            copy(r01.at[:, _ds(n, C)], add.at[slot, 1], dsem.at[slot, 1])]

    def d_out(n, slot):
        return copy(ob.at[slot], dx.at[pl.ds(0, T), _ds(n, C)], osem.at[slot])

    w_lhs(0, 2, 0)
    w_rhs(0, 2, 0)
    w_part(0)

    def w_step(grp, carry):
        unit, pos, k = w_of(grp)
        ls = grp % 2
        w_wait(ls)

        @pl.when(grp + 1 < n_w)
        def _():
            unit2, _, k2 = w_of(grp + 1)
            w_lhs(unit2, k2, 1 - ls)
            w_rhs(unit2, k2, 1 - ls)

        @pl.when(grp + 1 == n_w)
        def _():
            for c in (*d_lhs(0), *d_rhs(0, 0)):
                c.start()

        pl.when((k == 2) | (unit >= 4))(lambda: w_part_wait(pos))

        @pl.when((k == 3) & (pos < 5))
        def _():
            pl.when(pos > 1)(lambda: w_out_wait(pos + 1))
            w_part(pos + 1)
        for n in range(2):
            a = 2 * (pos % 3) + n
            acc[a] = _wgrad(acc[a], n, la.at[ls], wn.at[ls], lb.at[ls])
        pl.when(k == 3)(lambda: w_out(pos))
        return carry

    lax.fori_loop(0, n_w, w_step, 0)

    def d_step(n, carry):
        slot = n % 2

        @pl.when(n == 0)
        def _():
            for c in d_lhs(0):
                c.wait()
        for c in d_rhs(n, slot):
            c.wait()

        @pl.when(n < 3)
        def _():
            for c in d_rhs(n + 1, 1 - slot):
                c.start()
        pl.when(n >= 2)(lambda: d_out(n, slot).wait())
        p = sum(_dot(lhs[0, :, pl.ds(j * T, T)], wn[slot, pl.ds((2 * k + j) * C, C)], NT)
                for k, lhs in enumerate((la, lb)) for j in range(2))
        ob[slot] = (p + add[slot, 0].astype(F32) + add[slot, 1].astype(F32)).astype(BF16)
        d_out(n, slot).start()
        return carry

    lax.fori_loop(0, 4, d_step, 0)
    for s in range(2):
        d_out(2 + s, s).wait()
    for pos in range(3):
        w_out_wait(pos)


def _k3(dug, duu, wg, wu, psib, r23, _, dx, la, lb, wt, add, ob, lsem, rsem, dsem, osem):
    copy = pltpu.make_async_copy

    def lhs(m):
        return (copy(dug.at[_ds(2 + m, C)], la.at[m], lsem.at[m, 0]), copy(duu.at[_ds(2 + m, C)], lb.at[m], lsem.at[m, 1]))

    def rhs(n, slot):
        return (copy(wg.at[_ds(n, C)], wt.at[slot, 0], rsem.at[slot, 0]), copy(wu.at[_ds(n, C)], wt.at[slot, 1], rsem.at[slot, 1]))

    def adds(m, n, slot):
        return (copy(psib.at[_ds(2 + m, C), _ds(n, C)], add.at[slot, 0], dsem.at[slot, 0]),
                copy(r23.at[_ds(m, C), _ds(n, C)], add.at[slot, 1], dsem.at[slot, 1]))

    def out(m, n, slot):
        return copy(ob.at[slot], dx.at[_ds(2 + m, C), _ds(n, C)], osem.at[slot])

    for c in (*lhs(0), *rhs(0, 0), *adds(0, 0, 0), *lhs(1)):
        c.start()

    def step(i, carry):
        n, m, slot = i // 2, i % 2, i // 2 % 2

        @pl.when(i < 2)
        def _():
            for c in lhs(m):
                c.wait()

        @pl.when(m == 0)
        def _():
            for c in rhs(n, slot):
                c.wait()

            @pl.when(n < 3)
            def _():
                for c in rhs(n + 1, 1 - slot):
                    c.start()
        for c in adds(m, n, m):
            c.wait()

        @pl.when(i < 7)
        def _():
            for c in adds(1 - m, n + m, 1 - m):
                c.start()
        pl.when(i >= 2)(lambda: out(m, n, m).wait())
        p = _dot(la[m], wt[slot, 0], NT) + _dot(lb[m], wt[slot, 1], NT)
        ob[m] = (p + add[m, 0].astype(F32) + add[m, 1].astype(F32)).astype(BF16)
        out(m, n, m).start()
        return carry

    lax.fori_loop(0, 8, step, 0)
    for m in range(2):
        out(m, 3, m).wait()


def _local(x, dy, wg, wu, wd):
    def bf(r):
        return jax.ShapeDtypeStruct((r, S), BF16)

    def ff(r):
        return jax.ShapeDtypeStruct((r, S), F32)
    k1 = pl.pallas_call(
        _k1, name="gather_gate",
        out_shape=(bf(3 * S), bf(3 * S), bf(4 * S), bf(4 * S), bf(4 * S), bf(S), bf(T), bf(T), bf(T), ff(S), ff(S), ff(S)),
        in_specs=[ANY] * 5, out_specs=(ANY,) * 12,
        scratch_shapes=[pltpu.VMEM((2, T, S), BF16), pltpu.VMEM((2, T, S), BF16), pltpu.VMEM((2, S, T), BF16),
                        pltpu.VMEM((2, 2, C, S), BF16), pltpu.VMEM((2, 3, T, C), BF16), pltpu.VMEM((2, T, T), F32),
                        pltpu.VMEM((5, T, C), BF16), DMA((2, 4)), DMA((2, 4)), DMA((2, 3)), DMA((2,)),
                        DMA((8,)), DMA((8,)), DMA((16,)), DMA((16,)), DMA((8,)), DMA((8,)), DMA((2, 2)), DMA((16,)),
                        DMA((1,)), DMA((1,))],
        cost_estimate=pl.CostEstimate(flops=420_000_000_000, bytes_accessed=1 << 30, transcendentals=0),
        compiler_params=pltpu.CompilerParams(collective_id=0, has_side_effects=True, vmem_limit_bytes=VMEM))
    xa, dya, z, dug, duu, psib, _, s23, r01, pg, pu, pd = k1(x, dy, wg, wu, wd)
    r23 = lax.ppermute(s23, "tp", [(0, 2), (2, 0), (1, 3), (3, 1)])
    k2 = pl.pallas_call(
        _k2, name="wgrad_dx",
        out_shape=(ff(S), ff(S), ff(S), bf(S)),
        in_specs=[ANY] * 12, out_specs=(ANY,) * 4,
        scratch_shapes=[pltpu.VMEM((2, T, S), BF16), pltpu.VMEM((2, T, S), BF16), pltpu.VMEM((2, S, T), BF16),
                        pltpu.VMEM((2, T, C), BF16), pltpu.VMEM((6, T, T), F32),
                        pltpu.VMEM((2, 2, T, C), BF16), DMA((2, 2)), DMA((2, 4)), DMA((2,)), DMA((6,)), DMA((6,)), DMA((2, 2))],
        cost_estimate=pl.CostEstimate(flops=105_000_000_000, bytes_accessed=1 << 28, transcendentals=0),
        compiler_params=pltpu.CompilerParams(vmem_limit_bytes=VMEM))
    dwg, dwu, dwd, dx = k2(dya, xa, z, dug, duu, psib, r01, wg, wu, pg, pu, pd)
    dx = pl.pallas_call(
        _k3, name="dx", out_shape=bf(S), in_specs=[ANY] * 7, out_specs=ANY, input_output_aliases={6: 0},
        scratch_shapes=[pltpu.VMEM((2, C, S), BF16), pltpu.VMEM((2, C, S), BF16), pltpu.VMEM((2, 2, C, S), BF16),
                        pltpu.VMEM((2, 2, C, C), BF16), pltpu.VMEM((2, C, C), BF16), DMA((2, 2)), DMA((2, 2)), DMA((2, 2)), DMA((2,))],
        cost_estimate=pl.CostEstimate(flops=4 * T * S * S, bytes_accessed=1 << 25, transcendentals=0),
        compiler_params=pltpu.CompilerParams(vmem_limit_bytes=VMEM))(dug, duu, wg, wu, psib, r23, dx)
    return dx, dwg, dwu, dwd


def solution(mesh):
    rows = P(("dp", "tp"), None)
    return jax.shard_map(_local, mesh=mesh,
                         in_specs=(rows, rows, P(None, "tp"), P(None, "tp"), P("tp", None)),
                         out_specs=(rows, P("dp", "tp"), P("dp", "tp"), rows),
                         check_vma=False)
```
